128 devices in a mesh: prow: 8 (over z, y_lo), pcol: 16 (over x, y_hi, core).
Axes of the slice: x: 4, y: 4 (y_hi: 2, y_lo: 2; y = y_hi * 2 + y_lo), z: 4, core: 2. Of those that a mesh axis runs over, the one named last changes fastest.
Arguments:
- ainv_in: float32 [18, 8, 9, 16, 128, 128], P(None, 'prow', None, 'pcol'), as said below
- ufactor: bfloat16 [18, 8, 6, 128, 128], P(None, 'prow'), may hold values from -0.08984375 to 0.08984375
- dinv: float32 [6, 128, 128], replicated, may hold values from -6 to 6
- pattern: int32 [144, 144], replicated, may hold values from 0 to 1, as said below
Outputs:
- ainv_out: float32 [18, 8, 9, 16, 128, 128], P(None, 'prow', None, 'pcol')
The draws below stay inside these ranges and needn't reach their ends.
Inputs may be any that keep to these rules, and one draw needn't show every extreme that they name: For a column j below 6, pattern[i, j] is 0 for i <= j, 1 at the parent row (the nearest row below j that has a 1, at most 3 below j), and the other 1s of column j lie in rows where the parent's column has a 1; for j at least 6, pattern[i, j] is 1 exactly where i > j. `ainv_in`: a symmetric matrix.
All inputs are finite; a program needn't handle non-finite values.
Results may differ from the reference program's by a relative error of at most 0.0003.
Values may be sent and summed in bfloat16 or wider, within the bound.
No kernel may reach another device: no remote copies, remote signals or barrier semaphores. Data moves between devices by JAX's collectives and lax.ppermute only.
A program may use at most 128 MiB of HBM per device.

```python
import jax
import jax.numpy as jnp
from jax import lax

B = 128
NBLK = 144
NSTEP = 6
RB = 18
CB = 9
N_PROW = 8
N_PCOL = 16


def draw_ainv_in(key, part):
    order = NBLK * B
    noise = jax.random.normal(key, (order, order), jnp.float32)
    symmetric = (noise + noise.T) * (0.7 / (2.0 * order) ** 0.5)
    matrix = symmetric + 2.0 * jnp.eye(order, dtype=jnp.float32)
    return matrix.reshape(RB, NBLK // RB, B, CB, NBLK // CB, B).transpose(0, 1, 3, 4, 2, 5)


def draw_pattern(key, part):
    indices = jnp.arange(NBLK, dtype=jnp.int32)
    initial = ((indices[:, None] > indices[None, :]) & (indices[None, :] >= NSTEP)).astype(jnp.int32)

    def build(taken, current):
        column = NSTEP - 1 - taken
        local_key = jax.random.fold_in(jax.random.fold_in(key, 7), column)
        first_key, second_key = jax.random.split(local_key)
        jump_size = jax.random.randint(first_key, (), 1, 4, dtype=jnp.int32)
        parent = jnp.minimum(column + jump_size, NBLK - 1)
        keep_rows = jax.random.randint(second_key, (NBLK,), 0, 10, dtype=jnp.int32) < 9
        parent_col = lax.dynamic_index_in_dim(current, parent, 1, keepdims=False)
        new_col = (parent_col > 0) & keep_rows | (indices == parent)
        new_col = new_col & (indices > column)
        return lax.dynamic_update_index_in_dim(current, new_col.astype(jnp.int32), column, 1)
    return lax.fori_loop(0, NSTEP, build, initial)


def steps_of(stream_key, extent, shards, smallest, high):
    loudness, own = 1.0, jax.random.fold_in(stream_key, 6)
    for axis_at, shards_of in shards:
        heights = jnp.exp(jax.random.uniform(jax.random.fold_in(own, axis_at), (shards_of,), jnp.float32, smallest / len(shards), high / len(shards)))
        loudness = loudness * jnp.repeat(heights, extent[axis_at] // shards_of).reshape([-1 if axis == axis_at else 1 for axis in range(len(extent))])
    return loudness


def normal_values(stream_key, extent, deviation, reach, cuts=(), kind=jnp.bfloat16):
    drawn = jax.random.normal(stream_key, extent, jnp.float32) * deviation
    if len(cuts) > 0:
        drawn = steps_of(stream_key, extent, cuts, -0.22, 0.18) * drawn
    return jnp.clip(drawn, min=-reach, max=reach).astype(kind)


def setup_inputs(seed: int = 0) -> dict:
    streams_of = jax.random.split(jax.random.key(seed), 5)
    return {
        "ainv_in": draw_ainv_in(jax.random.fold_in(streams_of[4], 71), 0),
        "ufactor": normal_values(streams_of[1], (RB, N_PROW, NSTEP, B, B), 0.015, 0.08984375, ((1, 8),)),
        "dinv": normal_values(streams_of[2], (NSTEP, B, B), 1.0, 6.0, (), jnp.float32),
        "pattern": draw_pattern(jax.random.fold_in(streams_of[4], 71), 0),
    }


def dense_form(blocks):
    return blocks.transpose(0, 1, 4, 2, 3, 5).reshape(NBLK * B, NBLK * B)


def block_form(matrix):
    return matrix.reshape(RB, N_PROW, B, CB, N_PCOL, B).transpose(0, 1, 3, 4, 2, 5)


def reference(ainv_in, ufactor, dinv, pattern):
    matrix = dense_form(ainv_in)
    factor = ufactor.astype(jnp.float32)
    row_mask = jnp.repeat(pattern, B, axis=0).astype(jnp.float32)
    for taken in range(NSTEP):
        column = NSTEP - 1 - taken
        factor_col = factor[:, :, column].reshape(NBLK * B, B) * row_mask[:, column:column + 1]
        inverse_col = -jnp.dot(matrix, factor_col, precision=lax.Precision.HIGHEST) * row_mask[:, column:column + 1]
        diag_block = dinv[column] - jnp.dot(factor_col.T, inverse_col, precision=lax.Precision.HIGHEST)
        new_col = inverse_col.at[column * B:(column + 1) * B].set(diag_block)
        matrix = matrix.at[:, column * B:(column + 1) * B].set(new_col)
        matrix = matrix.at[column * B:(column + 1) * B, :].set(new_col.T)
    return block_form(matrix)
```

```python
import jax
import jax.numpy as jnp
from jax import lax
from jax.experimental import pallas as pl
from jax.experimental.pallas import tpu as pltpu
from jax.sharding import PartitionSpec as P

F32, BF16 = jnp.float32, jnp.bfloat16
GROUPS = ((0, 9),)
VMEM = pl.BlockSpec(memory_space=pltpu.VMEM)
SMEM = pl.BlockSpec(memory_space=pltpu.SMEM)
ANY = pl.BlockSpec(memory_space=pl.ANY)


def halves(value):
    high = value.astype(BF16)
    return high, (value - high.astype(F32)).astype(BF16)


def dot(left, right):
    return jnp.dot(left, right, preferred_element_type=F32)


def product_kernel(live, x_ref, u_ref, *refs):
    copy_ref, out_ref = refs[-2:]
    step = pl.program_id(0)
    rows, cols, width, _ = x_ref.shape
    steps = u_ref.shape[1]
    left, high, low = [], [], []
    for r in range(rows):
        wide = []
        for k in range(steps):
            block = u_ref[r, k]
            wide.append(jnp.where(live[step * rows + r, k] > 0, block, jnp.zeros_like(block)))
        left.append(jnp.concatenate(wide, axis=1))
        value = jnp.concatenate([x_ref[r, c] for c in range(cols)], axis=1)
        for c in range(cols):
            copy_ref[r, c] = x_ref[r, c]
        a, b = halves(value)
        high.append(a)
        low.append(b)
    left = jnp.concatenate(left, axis=0).T
    both = jnp.concatenate([left, left], axis=1)
    term = dot(both, jnp.concatenate(high + low, axis=0))
    term = term.reshape(out_ref.shape)

    @pl.when(step == 0)
    def _():
        out_ref[...] = term

    @pl.when(step > 0)
    def _():
        out_ref[...] += term


def products(blocks, lower, live, whole, first, cols, rows=2):
    row_blocks, _, width, _ = blocks.shape
    steps = lower.shape[1]
    flops = 4 * row_blocks * cols * steps * width**3
    group = first // cols
    known = [] if whole is None else [whole]
    return pl.pallas_call(
        product_kernel,
        grid_spec=pltpu.PrefetchScalarGridSpec(
            num_scalar_prefetch=1,
            grid=(row_blocks // rows,),
            in_specs=[
                pl.BlockSpec((rows, cols, width, width), lambda i, _: (i, group, 0, 0)),
                pl.BlockSpec((rows, steps, width, width), lambda i, _: (i, 0, 0, 0)),
            ]
            + [ANY] * len(known),
            out_specs=[
                pl.BlockSpec((rows, cols, width, width), lambda i, _: (i, group, 0, 0)),
                pl.BlockSpec((steps, width, cols * width), lambda i, _: (0, 0, 0)),
            ],
        ),
        out_shape=[
            jax.ShapeDtypeStruct(blocks.shape, F32),
            jax.ShapeDtypeStruct((steps, width, cols * width), F32),
        ],
        input_output_aliases={3: 0} if known else {},
        cost_estimate=pl.CostEstimate(
            flops=flops, bytes_accessed=8 * row_blocks * cols * width**2, transcendentals=0
        ),
        name="products",
    )(live, blocks, lower, *known)


def eliminate_kernel(live, p_ref, u_ref, out_ref):
    steps = p_ref.shape[0]
    high, low = [], []
    for k in reversed(range(steps)):
        total = p_ref[k]
        if high:
            blocks = []
            for j in range(k + 1, steps):
                block = u_ref[j, k]
                blocks.append(jnp.where(live[j, k] > 0, block, jnp.zeros_like(block)).T)
            left = jnp.concatenate(blocks + blocks, axis=1)
            total = total + dot(left, jnp.concatenate(high[::-1] + low[::-1], axis=0))
        total = -total
        out_ref[k] = total
        a, b = halves(total)
        high.append(a)
        low.append(b)


def eliminate(partial, corner, live):
    return pl.pallas_call(
        eliminate_kernel,
        in_specs=[SMEM, VMEM, VMEM],
        out_specs=VMEM,
        out_shape=jax.ShapeDtypeStruct(partial.shape, F32),
        cost_estimate=pl.CostEstimate(flops=1000 * partial.size, bytes_accessed=8 * partial.size, transcendentals=0),
        name="eliminate",
    )(live, partial, corner)


def column_kernel(live, *refs):
    *value_refs, u_ref, out_ref = refs
    _, steps, width, _ = u_ref.shape
    total, a = None, 0
    for even_ref, odd_ref in zip(value_refs[::2], value_refs[1::2]):
        for c in range(even_ref.shape[1] // width):
            part = pl.ds(c * width, width)
            value = jnp.concatenate([even_ref[:, part], odd_ref[:, part]], axis=1)
            left = jnp.concatenate(halves(value), axis=0)
            right = []
            for r in (a, a + 1):
                wide = []
                for k in range(steps):
                    block = u_ref[r, k]
                    wide.append(jnp.where(live[r, k] > 0, block, jnp.zeros_like(block)))
                right.append(jnp.concatenate(wide, axis=1))
            term = dot(left, jnp.concatenate(right, axis=0))
            total = term if total is None else total + term
            a += 2
    total = total[:width] + total[width:]
    out_ref[...] = total


def column_products(values, lower, live):
    row_blocks, steps, width, _ = lower.shape
    return pl.pallas_call(
        column_kernel,
        in_specs=[SMEM] + [VMEM] * (len(values) + 1),
        out_specs=VMEM,
        out_shape=jax.ShapeDtypeStruct((width, steps * width), F32),
        cost_estimate=pl.CostEstimate(flops=4 * row_blocks * steps * width**3, bytes_accessed=6 * 10**6, transcendentals=0),
        name="column",
    )(live, *values, lower)


def corner_kernel(info, live, h_ref, u_ref, dinv_ref, out_ref, x_ref):
    steps, width, _ = dinv_ref.shape
    for k in reversed(range(steps)):
        here = pl.ds(k * width, width)
        later = steps - 1 - k
        if later:
            right = []
            for j in range(k + 1, steps):
                block = u_ref[j, k]
                right.append(jnp.where(live[j, k] > 0, block, jnp.zeros_like(block)))
            right = jnp.concatenate(right, axis=0)
            both = jnp.concatenate([right, right], axis=0)
            rest = pl.ds((k + 1) * width, later * width)
            known = jnp.concatenate(halves(x_ref[rest, rest]), axis=1)
            value = dot(known, both)
            turned = []
            for i in range(k + 1, steps):
                at = (i - k - 1) * width
                block = -(value[at : at + width] + h_ref[info[2 + i], :, here])
                block = jnp.where(live[i, k] > 0, block, jnp.zeros_like(block))
                x_ref[pl.ds(i * width, width), here] = block
                turned.append(block.T)
            turned = jnp.concatenate(turned, axis=1)
            x_ref[here, rest] = turned
            tail = dot(jnp.concatenate(halves(turned), axis=1), both)
            x_ref[here, here] = dinv_ref[k].T - h_ref[info[2 + k], :, here] - tail
        else:
            x_ref[here, here] = dinv_ref[k].T - h_ref[info[2 + k], :, here]
    for k in range(steps):
        for j in range(steps):

            @pl.when((info[0] == k) & (info[1] == j))
            def _():
                out_ref[...] = x_ref[pl.ds(k * width, width), pl.ds(j * width, width)]


def corner_blocks(info, live, sums, corner, dinv):
    steps, width, _ = dinv.shape
    return pl.pallas_call(
        corner_kernel,
        in_specs=[SMEM, SMEM, VMEM, VMEM, VMEM],
        out_specs=VMEM,
        out_shape=jax.ShapeDtypeStruct((width, width), F32),
        scratch_shapes=[pltpu.VMEM((steps * width, steps * width), F32)],
        cost_estimate=pl.CostEstimate(flops=10**9, bytes_accessed=10**6, transcendentals=0),
        name="corner",
    )(info, live, sums, corner, dinv)


def patch_kernel(info, *refs):
    *value_refs, _, out_ref, turned_ref, sem_ref = refs
    row_blocks, cols, width, _ = out_ref.shape
    has_row, has_col, row_first, col_first = info[0], info[1], info[2], info[3]
    rows, columns = [], []
    for row_ref, even_ref, odd_ref in zip(value_refs[::3], value_refs[1::3], value_refs[2::3]):
        for c in range(row_ref.shape[1] // width):
            rows.append((row_ref, pl.ds(c * width, width)))
            columns.append((even_ref, pl.ds(c * width, width)))
            columns.append((odd_ref, pl.ds(c * width, width)))

    def row_copy(c):
        return pltpu.make_async_copy(rows[c][0].at[:, rows[c][1]], out_ref.at[0, c], sem_ref.at[c])

    def col_copy(a):
        return pltpu.make_async_copy(turned_ref.at[a], out_ref.at[a, 0], sem_ref.at[cols + a])

    @pl.when(has_row > 0)
    def _():
        for c in range(1, cols):
            row_copy(c).start()

    @pl.when(row_first > 0)
    def _():
        row_copy(0).start()

    @pl.when(has_col > 0)
    def _():
        for a in range(row_blocks):
            turned_ref[a] = columns[a][0][:, columns[a][1]].T
        for a in range(1, row_blocks):
            col_copy(a).start()
        for a in range(1, row_blocks):
            col_copy(a).wait()

    @pl.when(col_first > 0)
    def _():
        col_copy(0).start()
        col_copy(0).wait()

    @pl.when(has_row > 0)
    def _():
        for c in range(1, cols):
            row_copy(c).wait()

    @pl.when(row_first > 0)
    def _():
        row_copy(0).wait()


def patch(info, values, whole):
    row_blocks, cols, width, _ = whole.shape
    return pl.pallas_call(
        patch_kernel,
        in_specs=[SMEM] + [VMEM] * len(values) + [ANY],
        out_specs=ANY,
        out_shape=jax.ShapeDtypeStruct(whole.shape, F32),
        scratch_shapes=[pltpu.VMEM((row_blocks, width, width), F32), pltpu.SemaphoreType.DMA((row_blocks + cols,))],
        input_output_aliases={1 + len(values): 0},
        cost_estimate=pl.CostEstimate(flops=10**8, bytes_accessed=4 * 10**6, transcendentals=0),
        name="patch",
    )(info, *values, whole)


def first_kernel(info, block_ref, _, out_ref, sem_ref):
    @pl.when(info[0] > 0)
    def _():
        copy = pltpu.make_async_copy(block_ref, out_ref.at[0, 0], sem_ref)
        copy.start()
        copy.wait()


def patch_first(info, block, whole):
    return pl.pallas_call(
        first_kernel,
        in_specs=[SMEM, VMEM, ANY],
        out_specs=ANY,
        out_shape=jax.ShapeDtypeStruct(whole.shape, F32),
        scratch_shapes=[pltpu.SemaphoreType.DMA],
        input_output_aliases={2: 0},
        name="patch_first",
    )(info, block, whole)


def per_device(ainv_in, ufactor, dinv, pattern):
    row_blocks, _, cols, _, width, _ = ainv_in.shape
    steps = dinv.shape[0]
    n_row, n_col = lax.axis_size("prow"), lax.axis_size("pcol")
    blocks = ainv_in.reshape(row_blocks, cols, width, width)
    lower = ufactor.reshape(row_blocks, steps, width, width)
    p, q = lax.axis_index("prow"), lax.axis_index("pcol")
    z, y, core = p // 2, p % 2, q % 2
    n_z = n_row // 2
    row_ids = jnp.arange(row_blocks, dtype=jnp.int32) * n_row + p
    col_ids = jnp.arange(cols, dtype=jnp.int32) * n_col + q

    flags = pattern[:, :steps]
    mine = lax.dynamic_index_in_dim(flags.reshape(row_blocks, n_row, steps), p, 1, keepdims=False)
    live = ((mine > 0) & (row_ids >= steps)[:, None]).astype(jnp.int32)
    live_corner = flags[:steps]
    mine = lax.dynamic_index_in_dim(flags.reshape(cols, n_col, steps), q, 1, keepdims=False)
    mine = lax.dynamic_index_in_dim(mine, jnp.minimum(p, steps - 1), 1, keepdims=False)
    row_live = (mine > 0) & (col_ids >= steps)

    def at(zz, yy):
        return zz % n_z * 2 + yy

    flip_y = [(d, d ^ 1) for d in range(n_row)]
    flip_z = [(d, d ^ 2) for d in range(n_row)]
    mirror = [(d, at(n_z - 1 - d // 2, d % 2)) for d in range(n_row)]
    flip_core = [(d, d ^ 1) for d in range(n_col)]

    half = width // 2
    mine = lax.dynamic_slice_in_dim(lower[0], core * half, half, axis=1)

    def join(bit, own, other):
        return jnp.where(bit == 0, jnp.concatenate([own, other]), jnp.concatenate([other, own]))

    with jax.named_scope("corner_u"):
        got = mine[None]
        got = join(y, got, lax.ppermute(got, "prow", flip_y))
        got = join(z % 2, got, lax.ppermute(got, "prow", flip_z))
        got = join(z // 2, got, lax.ppermute(got, "prow", mirror))[:steps]
        other = lax.ppermute(got, "pcol", flip_core)
        corner = jnp.where(core == 0, jnp.concatenate([got, other], axis=2), jnp.concatenate([other, got], axis=2))

    n_dest = steps // 2

    def ring(shift, ok):
        return [(at(zz, yy), at(zz + shift, yy)) for zz in range(n_z) for yy in range(2) if ok(zz)]

    def near(shift):
        return ring(shift, lambda zz: (zz + shift) % n_z < n_dest)

    def far(shift):
        return ring(shift, lambda zz: (zz + 2 * shift) % n_z < n_dest)

    flip_owners = [(d, d ^ 1) for d in range(n_row) if d ^ 1 < steps]

    def route(group):
        return [(k * n_col + d + group * n_row, d * n_col + k) for k in range(steps) for d in range(n_row)]

    whole, values = None, []
    for first, count in GROUPS:
        whole, partial = products(blocks, lower, live, whole, first, count)
        partial = eliminate(partial, corner, live_corner)
        pairs = partial.reshape(n_dest, 2, width, count * width)

        def piece(zz, par):
            zz = jnp.minimum(zz % n_z, n_dest - 1)
            return lax.dynamic_index_in_dim(pairs, zz, 0, keepdims=False)[par]

        with jax.named_scope("reduce_z"):
            far_up = lax.ppermute(piece(z + 2, 0), "prow", far(1))
            far_down = lax.ppermute(piece(z + 2, 1), "prow", far(-1))
            near_up1 = lax.ppermute(piece(z + 1, 1), "prow", near(1))
            near_down1 = lax.ppermute(piece(z - 1, 0), "prow", near(-1))
            near_up2 = lax.ppermute(piece(z + 1, 0) + far_up, "prow", near(1))
            near_down2 = lax.ppermute(piece(z - 1, 1) + far_down, "prow", near(-1))
            even = piece(z, 0) + near_down1 + near_up2
            odd = piece(z, 1) + near_up1 + near_down2
        with jax.named_scope("reduce_y"):
            keep, give = jnp.where(y == 0, even, odd), jnp.where(y == 0, odd, even)
            full = keep + lax.ppermute(give, "prow", flip_owners)
        mask = jnp.broadcast_to(row_live[first : first + count, None], (count, width))
        row = jnp.where(mask.reshape(1, count * width), full, jnp.zeros_like(full))
        with jax.named_scope("forward"):
            even = lax.ppermute(row, ("prow", "pcol"), route(0))
            odd = lax.ppermute(row, ("prow", "pcol"), route(1))
        values.append((row, even, odd))

    sums = column_products([v for _, *pair in values for v in pair], lower, live)
    with jax.named_scope("corner_sum"):
        for perm in (flip_y, flip_z, mirror):
            sums = sums + lax.ppermute(sums, "prow", perm)
        turns = [lax.ppermute(sums, "pcol", [(d, (d + t) % steps) for d in range(steps)]) for t in (2, 4)]
        same = jnp.stack([sums, *turns])
        mates = lax.ppermute(same, "pcol", [(d, d ^ 1) for d in range(steps)])
        sums = jnp.concatenate([same, mates])

    has_row, has_col = p < steps, q < steps
    info = jnp.stack([has_row, has_col, has_row & ~has_col, has_col & ~has_row]).astype(jnp.int32)
    whole = patch(info, [v for group in values for v in group], whole)
    ks = jnp.arange(steps, dtype=jnp.int32)
    slots = (q // 2 - ks // 2) % n_dest + n_dest * ((ks % 2) ^ (q % 2))
    info = jnp.concatenate([jnp.stack([p, q]), slots]).astype(jnp.int32)
    block = corner_blocks(info, live_corner, sums, corner, dinv)
    info = jnp.stack([has_row & has_col]).astype(jnp.int32)
    whole = patch_first(info, block, whole)
    return whole.reshape(ainv_in.shape)


def solution(mesh):
    placed = (
        P(None, "prow", None, "pcol", None, None),
        P(None, "prow", None, None, None),
        P(),
        P(),
    )
    return jax.shard_map(
        per_device,
        mesh=mesh,
        in_specs=placed,
        out_specs=P(None, "prow", None, "pcol", None, None),
        check_vma=False,
    )
```

```python
import jax
import jax.numpy as jnp
from jax import lax
from jax.experimental import pallas as pl
from jax.experimental.pallas import tpu as pltpu
from jax.sharding import PartitionSpec as P


F32, BF16 = jnp.float32, jnp.bfloat16
PARTS = ((0, 8), (8, 10))
VMEM = pl.BlockSpec(memory_space=pltpu.VMEM)
SMEM = pl.BlockSpec(memory_space=pltpu.SMEM)
ANY = pl.BlockSpec(memory_space=pl.ANY)


def halves(value):
    high = value.astype(BF16)
    return high, (value - high.astype(F32)).astype(BF16)


def stacked(core, own, other):
    return jnp.concatenate([jnp.where(core > 0, other, own), jnp.where(core > 0, own, other)], axis=0)


def dot(left, right):
    return jnp.dot(left, right, preferred_element_type=F32)


def product_kernel(live, x_ref, u_ref, *refs):
    copy_ref, out_ref = refs[-2:]
    step = pl.program_id(0)
    rows, cols, _, _ = x_ref.shape
    steps = u_ref.shape[1]
    left, high, low = [], [], []
    for r in range(rows):
        wide = []
        for k in range(steps):
            block = u_ref[r, k]
            wide.append(jnp.where(live[step * rows + r, k] > 0, block, jnp.zeros_like(block)))
        left.append(jnp.concatenate(wide, axis=1))
        value = jnp.concatenate([x_ref[r, c] for c in range(cols)], axis=1)
        for c in range(cols):
            copy_ref[r, c] = x_ref[r, c]
        a, b = halves(value)
        high.append(a)
        low.append(b)
    left = jnp.concatenate(left, axis=0).T
    both = jnp.concatenate([left, left], axis=1)
    term = dot(both, jnp.concatenate(high + low, axis=0))
    term = term.reshape(out_ref.shape)

    @pl.when(step == 0)
    def _():
        out_ref[...] = term

    @pl.when(step > 0)
    def _():
        out_ref[...] += term


def products(blocks, lower, live, whole, first, count, rows=2):
    _, cols, width, _ = blocks.shape
    steps = lower.shape[1]
    start = first // rows
    known = [] if whole is None else [whole]
    return pl.pallas_call(
        product_kernel,
        grid_spec=pltpu.PrefetchScalarGridSpec(
            num_scalar_prefetch=1,
            grid=(count // rows,),
            in_specs=[
                pl.BlockSpec((rows, cols, width, width), lambda i, _: (start + i, 0, 0, 0)),
                pl.BlockSpec((rows, steps, width, width), lambda i, _: (start + i, 0, 0, 0)),
            ]
            + [ANY] * len(known),
            out_specs=[
                pl.BlockSpec((rows, cols, width, width), lambda i, _: (start + i, 0, 0, 0)),
                pl.BlockSpec((steps, width, cols * width), lambda i, _: (0, 0, 0)),
            ],
        ),
        out_shape=[
            jax.ShapeDtypeStruct(blocks.shape, F32),
            jax.ShapeDtypeStruct((steps, width, cols * width), F32),
        ],
        input_output_aliases={3: 0} if known else {},
        cost_estimate=pl.CostEstimate(
            flops=4 * count * cols * steps * width**3, bytes_accessed=8 * count * cols * width**2, transcendentals=0
        ),
        name="products",
    )(live[first : first + count], blocks, lower, *known)


def eliminate_kernel(take, live, *refs):
    *part_refs, u_ref, v_ref, up_ref, down_ref, up2_ref, down2_ref, own_ref, w_ref = refs
    steps = w_ref.shape[0]
    high, low = [], []
    for k in reversed(range(steps)):
        total = part_refs[0][k]
        for ref in part_refs[1:]:
            total = total + ref[k]
        if high:
            blocks = []
            for j in range(k + 1, steps):
                block = stacked(take[8], u_ref[j, k], v_ref[j, k])
                blocks.append(jnp.where(live[j, k] > 0, block, jnp.zeros_like(block)).T)
            left = jnp.concatenate(blocks + blocks, axis=1)
            total = total + dot(left, jnp.concatenate(high[::-1] + low[::-1], axis=0))
        total = -total
        w_ref[k] = total
        a, b = halves(total)
        high.append(a)
        low.append(b)
    places = [up_ref.at[0], up_ref.at[1], down_ref.at[0], down_ref.at[1], up2_ref, down2_ref, own_ref.at[0], own_ref.at[1]]
    for n, place in enumerate(places):
        place[...] = w_ref[take[n]]


def eliminate(parts, corner, live, take):
    _, width, wide = parts[0].shape
    one = jax.ShapeDtypeStruct((width, wide), F32)
    two = jax.ShapeDtypeStruct((2, width, wide), F32)
    return pl.pallas_call(
        eliminate_kernel,
        in_specs=[SMEM, SMEM] + [VMEM] * (len(parts) + 2),
        out_specs=[VMEM] * 5,
        out_shape=[two, two, one, one, two],
        scratch_shapes=[pltpu.VMEM(parts[0].shape, F32)],
        cost_estimate=pl.CostEstimate(flops=1000 * parts[0].size, bytes_accessed=20 * parts[0].size, transcendentals=0),
        name="eliminate",
    )(take, live, *parts, *corner)


def column_kernel(info, live, row_ref, near_ref, far_ref, out_ref):
    cols, steps, width, _ = near_ref.shape
    total = None
    for c in range(0, cols, 2):
        count = min(2, cols - c)
        left = jnp.concatenate(halves(row_ref[:, pl.ds(c * width, count * width)]), axis=0)
        right = []
        for r in range(c, c + count):
            wide = []
            for k in range(steps):
                block = jnp.where(info[0] > 0, near_ref[r, k], far_ref[r, k])
                wide.append(jnp.where(live[r, k] > 0, block, jnp.zeros_like(block)))
            right.append(jnp.concatenate(wide, axis=1))
        term = dot(left, jnp.concatenate(right, axis=0))
        total = term if total is None else total + term
    out_ref[...] = total[:width] + total[width:]


def column_products(info, live, row, near, far):
    cols, steps, width, _ = near.shape
    return pl.pallas_call(
        column_kernel,
        in_specs=[SMEM, SMEM, VMEM, VMEM, VMEM],
        out_specs=VMEM,
        out_shape=jax.ShapeDtypeStruct((width, steps * width), F32),
        cost_estimate=pl.CostEstimate(flops=4 * cols * steps * width**3, bytes_accessed=6 * 10**6, transcendentals=0),
        name="column",
    )(info, live, row, near, far)


def corner_kernel(info, live, g_ref, h_ref, u_ref, v_ref, dinv_ref, out_ref, x_ref):
    steps, width, _ = dinv_ref.shape
    for k in reversed(range(steps)):
        here = pl.ds(k * width, width)
        later = steps - 1 - k
        if later:
            right = []
            for j in range(k + 1, steps):
                block = stacked(info[2], u_ref[j, k], v_ref[j, k])
                right.append(jnp.where(live[j, k] > 0, block, jnp.zeros_like(block)))
            right = jnp.concatenate(right, axis=0)
            both = jnp.concatenate([right, right], axis=0)
            rest = pl.ds((k + 1) * width, later * width)
            known = jnp.concatenate(halves(x_ref[rest, rest]), axis=1)
            value = dot(known, both)
            turned = []
            for i in range(k + 1, steps):
                at = (i - k - 1) * width
                block = -(value[at : at + width] + stacked(info[2], g_ref[i, :, here], h_ref[i, :, here]))
                block = jnp.where(live[i, k] > 0, block, jnp.zeros_like(block))
                x_ref[pl.ds(i * width, width), here] = block
                turned.append(block.T)
            turned = jnp.concatenate(turned, axis=1)
            x_ref[here, rest] = turned
            tail = dot(jnp.concatenate(halves(turned), axis=1), both)
            x_ref[here, here] = dinv_ref[k].T - stacked(info[2], g_ref[k, :, here], h_ref[k, :, here]) - tail
        else:
            x_ref[here, here] = dinv_ref[k].T - stacked(info[2], g_ref[k, :, here], h_ref[k, :, here])
    for k in range(steps):
        for j in range(steps):

            @pl.when((info[0] == k) & (info[1] == j))
            def _():
                out_ref[...] = x_ref[pl.ds(k * width, width), pl.ds(j * width, width)]


def corner_blocks(info, live, sums, corner, dinv):
    steps, width, _ = dinv.shape
    return pl.pallas_call(
        corner_kernel,
        in_specs=[SMEM, SMEM] + [VMEM] * 5,
        out_specs=VMEM,
        out_shape=jax.ShapeDtypeStruct((width, width), F32),
        scratch_shapes=[pltpu.VMEM((steps * width, steps * width), F32)],
        cost_estimate=pl.CostEstimate(flops=10**9, bytes_accessed=10**6, transcendentals=0),
        name="corner",
    )(info, live, *sums, *corner, dinv)


def patch_kernel(info, *refs):
    *value_refs, _, out_ref, turned_ref, sem_ref = refs
    row_blocks, cols, width, _ = out_ref.shape
    has_row, has_col, row_first, col_first = info[0], info[1], info[2], info[3]
    rows, columns = [], []
    for row_ref, even_ref, odd_ref in zip(value_refs[::3], value_refs[1::3], value_refs[2::3]):
        for c in range(row_ref.shape[1] // width):
            rows.append((row_ref, pl.ds(c * width, width)))
            columns.append((even_ref, pl.ds(c * width, width)))
            columns.append((odd_ref, pl.ds(c * width, width)))

    def row_copy(c):
        return pltpu.make_async_copy(rows[c][0].at[:, rows[c][1]], out_ref.at[0, c], sem_ref.at[c])

    def col_copy(a):
        return pltpu.make_async_copy(turned_ref.at[a], out_ref.at[a, 0], sem_ref.at[cols + a])

    @pl.when(has_row > 0)
    def _():
        for c in range(1, cols):
            row_copy(c).start()

    @pl.when(row_first > 0)
    def _():
        row_copy(0).start()

    @pl.when(has_col > 0)
    def _():
        for a in range(row_blocks):
            turned_ref[a] = columns[a][0][:, columns[a][1]].T
        for a in range(1, row_blocks):
            col_copy(a).start()
        for a in range(1, row_blocks):
            col_copy(a).wait()

    @pl.when(col_first > 0)
    def _():
        col_copy(0).start()
        col_copy(0).wait()

    @pl.when(has_row > 0)
    def _():
        for c in range(1, cols):
            row_copy(c).wait()

    @pl.when(row_first > 0)
    def _():
        row_copy(0).wait()


def patch(info, values, whole):
    row_blocks, cols, width, _ = whole.shape
    return pl.pallas_call(
        patch_kernel,
        in_specs=[SMEM] + [VMEM] * len(values) + [ANY],
        out_specs=ANY,
        out_shape=jax.ShapeDtypeStruct(whole.shape, F32),
        scratch_shapes=[pltpu.VMEM((row_blocks, width, width), F32), pltpu.SemaphoreType.DMA((row_blocks + cols,))],
        input_output_aliases={1 + len(values): 0},
        cost_estimate=pl.CostEstimate(flops=10**8, bytes_accessed=4 * 10**6, transcendentals=0),
        name="patch",
    )(info, *values, whole)


def first_kernel(info, block_ref, _, out_ref, sem_ref):
    @pl.when(info[0] > 0)
    def _():
        copy = pltpu.make_async_copy(block_ref, out_ref.at[0, 0], sem_ref)
        copy.start()
        copy.wait()


def patch_first(info, block, whole):
    return pl.pallas_call(
        first_kernel,
        in_specs=[SMEM, VMEM, ANY],
        out_specs=ANY,
        out_shape=jax.ShapeDtypeStruct(whole.shape, F32),
        scratch_shapes=[pltpu.SemaphoreType.DMA],
        input_output_aliases={2: 0},
        name="patch_first",
    )(info, block, whole)


def per_device(ainv_in, ufactor, dinv, pattern):
    row_blocks, _, cols, _, width, _ = ainv_in.shape
    steps = dinv.shape[0]
    n_row, n_col = lax.axis_size("prow"), lax.axis_size("pcol")
    blocks = ainv_in.reshape(row_blocks, cols, width, width)
    lower = ufactor.reshape(row_blocks, steps, width, width)
    p, q = lax.axis_index("prow"), lax.axis_index("pcol")
    z, y, core = p // 2, p % 2, q % 2
    n_z = n_row // 2
    row_ids = jnp.arange(row_blocks, dtype=jnp.int32) * n_row + p
    col_ids = jnp.arange(cols, dtype=jnp.int32) * n_col + q

    flags = pattern[:, :steps]
    mine = lax.dynamic_index_in_dim(flags.reshape(row_blocks, n_row, steps), p, 1, keepdims=False)
    live = ((mine > 0) & (row_ids >= steps)[:, None]).astype(jnp.int32)
    live_corner = flags[:steps]
    mine = lax.dynamic_index_in_dim(flags.reshape(cols, n_col, steps), q, 1, keepdims=False)
    live_cols = ((mine > 0) & (col_ids >= steps)[:, None]).astype(jnp.int32)
    row_live = lax.dynamic_index_in_dim(live_cols, jnp.minimum(p, steps - 1), 1, keepdims=False) > 0

    def at(zz, yy):
        return zz % n_z * 2 + yy

    flip_y = [(d, d ^ 1) for d in range(n_row)]
    flip_z = [(d, d ^ 2) for d in range(n_row)]
    mirror = [(d, at(n_z - 1 - d // 2, d % 2)) for d in range(n_row)]
    flip_core = [(d, d ^ 1) for d in range(n_col)]

    half = width // 2
    mine = lax.dynamic_slice_in_dim(lower[0], core * half, half, axis=1)

    def join(bit, own, other):
        return jnp.where(bit == 0, jnp.concatenate([own, other]), jnp.concatenate([other, own]))

    def ring(shift):
        return [(at(zz, yy), at(zz + shift, yy)) for zz in range(n_z) for yy in range(2)]

    pair = join(y, mine[None], lax.ppermute(mine[None], "prow", flip_y))
    moved = [pair] + [lax.ppermute(pair, "prow", ring(shift)) for shift in (1, 2, 3)]
    corner = []
    for t in range(steps // 2):
        away = (z - t) % n_z
        corner.append(jnp.where(away == 0, moved[0], jnp.where(away == 1, moved[1], jnp.where(away == 2, moved[2], moved[3]))))
    corner = jnp.concatenate(corner)
    corner = corner, lax.ppermute(corner, "pcol", flip_core)

    n_dest = steps // 2

    both, grid = ("prow", "pcol"), [(x, h, c) for x in range(n_col // 4) for h in range(2) for c in range(2)]

    def device(x, h, c, zz, yy):
        return at(zz, yy) * n_col + x * 4 + h * 2 + c

    def source(x, h):
        return x % 2 * 2 + h

    mine = lower.reshape(cols, 2, steps, width, width)
    mine = lax.dynamic_index_in_dim(mine, q // n_row, 1, keepdims=False)
    ahead = [(device(x, h, c, source(x, h), c), device(x, h, c, source(x, h) + 1, c)) for x, h, c in grid]
    behind = [(device(x, h, 1 - c, source(x, h), c), device(x, h, c, source(x, h) + 3, c)) for x, h, c in grid]
    from_behind = lax.ppermute(mine, both, ahead)
    from_ahead = lax.ppermute(mine, both, behind)
    cut = (cols + 1) // 2
    ahead = [(device(x, h, c, source(x, h) + 1, c), device(x, h, c, source(x, h) + 2, c)) for x, h, c in grid]
    behind = [(device(x, h, c, source(x, h) + 3, c), device(x, h, c, source(x, h) + 2, c)) for x, h, c in grid]
    opposite = jnp.concatenate(
        [lax.ppermute(from_behind[:cut], both, ahead), lax.ppermute(from_ahead[cut:], both, behind)]
    )
    apart = (z - (q // 4 % 2 * 2 + q // 2 % 2)) % n_z
    near_u = jnp.where(
        apart == 0, mine, jnp.where(apart == 1, from_behind, jnp.where(apart == 3, from_ahead, opposite))
    )
    across = [
        (device(x, h, c, zz, c), device(x, h, c, zz, 1 - c)) for x, h, c in grid for zz in range(n_dest)
    ]
    far_u = lax.ppermute(near_u, both, across)

    whole, parts = None, []
    for first, count in PARTS:
        whole, part = products(blocks, lower, live, whole, first, count)
        parts.append(part)

    def near(shift):
        return [(s, d) for s, d in ring(shift) if d < steps]

    def slot(zz, par):
        return jnp.minimum(zz % n_z, n_dest - 1) * 2 + par

    take = [slot(z + 2, 0), slot(z + 1, 1), slot(z + 2, 1), slot(z - 1, 0)]
    take += [slot(z + 1, 0), slot(z - 1, 1), slot(z, 0), slot(z, 1), core]
    up, down, up2, down2, own = eliminate(parts, corner, live_corner, jnp.stack(take).astype(jnp.int32))
    up = lax.ppermute(up, "prow", ring(1))
    down = lax.ppermute(down, "prow", ring(-1))
    up2 = lax.ppermute(up2 + up[0], "prow", near(1))
    down2 = lax.ppermute(down2 + down[0], "prow", near(-1))
    even, odd = own[0] + down[1] + up2, own[1] + up[1] + down2
    keep, give = jnp.where(y == 0, even, odd), jnp.where(y == 0, odd, even)
    full = keep + lax.ppermute(give, "prow", [(d, d ^ 1) for d in range(steps)])
    mask = jnp.broadcast_to(row_live[:, None], (cols, width)).reshape(1, cols * width)
    row = jnp.where(mask, full, jnp.zeros_like(full))

    def route(group):
        return [(k * n_col + d + group * n_row, d * n_col + k) for k in range(steps) for d in range(n_row)]

    values = [row, lax.ppermute(row, both, route(0)), lax.ppermute(row, both, route(1))]

    sums = column_products((y == core).astype(jnp.int32).reshape(1), live_cols, row, near_u, far_u)
    parts = sums.reshape(2, half, steps * width)
    keep = lax.dynamic_index_in_dim(parts, core, 0, keepdims=False)
    give = lax.dynamic_index_in_dim(parts, 1 - core, 0, keepdims=False)
    got = keep + lax.ppermute(give, "pcol", flip_core)
    got = got + lax.ppermute(got, "pcol", [(d, d ^ 2) for d in range(n_col)])
    got = got + lax.ppermute(got, "pcol", [(d, d ^ 4) for d in range(n_col)])
    got = got + lax.ppermute(got, "pcol", [(d, (n_col // 4 - 1 - d // 4) * 4 + d % 4) for d in range(n_col)])

    def here(perm):
        return [(s * n_col + d, t * n_col + d) for s, t in perm for d in range(steps)]

    got = got[None]
    got = join(y, got, lax.ppermute(got, both, here(flip_y)))
    got = join(z % 2, got, lax.ppermute(got, both, here(flip_z)))
    last = steps - 4
    rise = lax.ppermute(got, both, here([(s, t) for s, t in mirror if s < 4]))
    fall = lax.ppermute(got[:last], both, here([(s, t) for s, t in mirror if s >= 4]))
    upper = z // 2 == 1
    got = jnp.concatenate([jnp.where(upper, rise, got), jnp.where(upper, got[:last], fall)])
    other = lax.ppermute(got, "pcol", [(d, d ^ 1) for d in range(steps)])
    sums = got, other

    has_row, has_col = p < steps, q < steps
    info = jnp.stack([has_row, has_col, has_row & ~has_col, has_col & ~has_row]).astype(jnp.int32)
    whole = patch(info, values, whole)
    info = jnp.stack([p, q, core]).astype(jnp.int32)
    block = corner_blocks(info, live_corner, sums, corner, dinv)
    info = jnp.stack([has_row & has_col]).astype(jnp.int32)
    whole = patch_first(info, block, whole)
    return whole.reshape(ainv_in.shape)


def solution(mesh):
    placed = (
        P(None, "prow", None, "pcol", None, None),
        P(None, "prow", None, None, None),
        P(),
        P(),
    )
    return jax.shard_map(
        per_device,
        mesh=mesh,
        in_specs=placed,
        out_specs=P(None, "prow", None, "pcol", None, None),
        check_vma=False,
    )
```

```python
import jax
import jax.numpy as jnp
from jax import lax
from jax.experimental import pallas as pl
from jax.experimental.pallas import tpu as pltpu
from jax.sharding import PartitionSpec as P


F32, BF16 = jnp.float32, jnp.bfloat16
PARTS = ((0, 8), (8, 10))
VMEM = pl.BlockSpec(memory_space=pltpu.VMEM)
SMEM = pl.BlockSpec(memory_space=pltpu.SMEM)
ANY = pl.BlockSpec(memory_space=pl.ANY)


def halves(value):
    high = value.astype(BF16)
    return high, (value - high.astype(F32)).astype(BF16)


def stacked(core, own, other):
    return jnp.concatenate([jnp.where(core > 0, other, own), jnp.where(core > 0, own, other)], axis=0)


def dot(left, right):
    return jnp.dot(left, right, preferred_element_type=F32)


def product_kernel(live, x_ref, u_ref, *refs):
    copy_ref, out_ref = refs[-2:]
    step = pl.program_id(0)
    rows, cols, _, _ = x_ref.shape
    steps = u_ref.shape[1]
    left, high, low = [], [], []
    for r in range(rows):
        wide = []
        for k in range(steps):
            block = u_ref[r, k]
            wide.append(jnp.where(live[step * rows + r, k] > 0, block, jnp.zeros_like(block)))
        left.append(jnp.concatenate(wide, axis=1))
        value = jnp.concatenate([x_ref[r, c] for c in range(cols)], axis=1)
        for c in range(cols):
            copy_ref[r, c] = x_ref[r, c]
        a, b = halves(value)
        high.append(a)
        low.append(b)
    left = jnp.concatenate(left, axis=0).T
    both = jnp.concatenate([left, left], axis=1)
    term = dot(both, jnp.concatenate(high + low, axis=0))
    term = term.reshape(out_ref.shape)

    @pl.when(step == 0)
    def _():
        out_ref[...] = term

    @pl.when(step > 0)
    def _():
        out_ref[...] += term


def products(blocks, lower, live, whole, first, count, rows=2):
    _, cols, width, _ = blocks.shape
    steps = lower.shape[1]
    start = first // rows
    known = [] if whole is None else [whole]
    return pl.pallas_call(
        product_kernel,
        grid_spec=pltpu.PrefetchScalarGridSpec(
            num_scalar_prefetch=1,
            grid=(count // rows,),
            in_specs=[
                pl.BlockSpec((rows, cols, width, width), lambda i, _: (start + i, 0, 0, 0)),
                pl.BlockSpec((rows, steps, width, width), lambda i, _: (start + i, 0, 0, 0)),
            ]
            + [ANY] * len(known),
            out_specs=[
                pl.BlockSpec((rows, cols, width, width), lambda i, _: (start + i, 0, 0, 0)),
                pl.BlockSpec((steps, width, cols * width), lambda i, _: (0, 0, 0)),
            ],
        ),
        out_shape=[
            jax.ShapeDtypeStruct(blocks.shape, F32),
            jax.ShapeDtypeStruct((steps, width, cols * width), F32),
        ],
        input_output_aliases={3: 0} if known else {},
        cost_estimate=pl.CostEstimate(
            flops=4 * count * cols * steps * width**3, bytes_accessed=8 * count * cols * width**2, transcendentals=0
        ),
        name="products",
    )(live[first : first + count], blocks, lower, *known)


def eliminate_kernel(take, live, *refs):
    *part_refs, u_ref, v_ref, up_ref, down_ref, up2_ref, down2_ref, own_ref, w_ref = refs
    steps = w_ref.shape[0]
    high, low = [], []
    for k in reversed(range(steps)):
        total = part_refs[0][k]
        for ref in part_refs[1:]:
            total = total + ref[k]
        if high:
            blocks = []
            for j in range(k + 1, steps):
                block = stacked(take[8], u_ref[j, k], v_ref[j, k])
                blocks.append(jnp.where(live[j, k] > 0, block, jnp.zeros_like(block)).T)
            left = jnp.concatenate(blocks + blocks, axis=1)
            total = total + dot(left, jnp.concatenate(high[::-1] + low[::-1], axis=0))
        total = -total
        w_ref[k] = total
        a, b = halves(total)
        high.append(a)
        low.append(b)
    places = [up_ref.at[0], up_ref.at[1], down_ref.at[0], down_ref.at[1], up2_ref, down2_ref, own_ref.at[0], own_ref.at[1]]
    for n, place in enumerate(places):
        place[...] = w_ref[take[n]]


def eliminate(parts, corner, live, take):
    _, width, wide = parts[0].shape
    one = jax.ShapeDtypeStruct((width, wide), F32)
    two = jax.ShapeDtypeStruct((2, width, wide), F32)
    return pl.pallas_call(
        eliminate_kernel,
        in_specs=[SMEM, SMEM] + [VMEM] * (len(parts) + 2),
        out_specs=[VMEM] * 5,
        out_shape=[two, two, one, one, two],
        scratch_shapes=[pltpu.VMEM(parts[0].shape, F32)],
        cost_estimate=pl.CostEstimate(flops=1000 * parts[0].size, bytes_accessed=20 * parts[0].size, transcendentals=0),
        name="eliminate",
    )(take, live, *parts, *corner)


def column_kernel(live, *refs):
    *value_refs, u_ref, out_ref = refs
    _, steps, width, _ = u_ref.shape
    total, a = None, 0
    for even_ref, odd_ref in zip(value_refs[::2], value_refs[1::2]):
        for c in range(even_ref.shape[1] // width):
            part = pl.ds(c * width, width)
            value = jnp.concatenate([even_ref[:, part], odd_ref[:, part]], axis=1)
            left = jnp.concatenate(halves(value), axis=0)
            right = []
            for r in (a, a + 1):
                wide = []
                for k in range(steps):
                    block = u_ref[r, k]
                    wide.append(jnp.where(live[r, k] > 0, block, jnp.zeros_like(block)))
                right.append(jnp.concatenate(wide, axis=1))
            term = dot(left, jnp.concatenate(right, axis=0))
            total = term if total is None else total + term
            a += 2
    total = total[:width] + total[width:]
    out_ref[...] = total


def column_products(values, lower, live):
    row_blocks, steps, width, _ = lower.shape
    return pl.pallas_call(
        column_kernel,
        in_specs=[SMEM] + [VMEM] * (len(values) + 1),
        out_specs=VMEM,
        out_shape=jax.ShapeDtypeStruct((width, steps * width), F32),
        cost_estimate=pl.CostEstimate(flops=4 * row_blocks * steps * width**3, bytes_accessed=6 * 10**6, transcendentals=0),
        name="column",
    )(live, *values, lower)


def corner_kernel(info, live, *refs):
    *sum_refs, u_ref, v_ref, dinv_ref, out_ref, x_ref, h_ref = refs
    steps, width, _ = dinv_ref.shape
    for n, ref in enumerate(sum_refs):
        h_ref[info[3 + n]] = ref[...]
    for k in reversed(range(steps)):
        here = pl.ds(k * width, width)
        later = steps - 1 - k
        if later:
            right = []
            for j in range(k + 1, steps):
                block = stacked(info[2], u_ref[j, k], v_ref[j, k])
                right.append(jnp.where(live[j, k] > 0, block, jnp.zeros_like(block)))
            right = jnp.concatenate(right, axis=0)
            both = jnp.concatenate([right, right], axis=0)
            rest = pl.ds((k + 1) * width, later * width)
            known = jnp.concatenate(halves(x_ref[rest, rest]), axis=1)
            value = dot(known, both)
            turned = []
            for i in range(k + 1, steps):
                at = (i - k - 1) * width
                block = -(value[at : at + width] + h_ref[i, :, here])
                block = jnp.where(live[i, k] > 0, block, jnp.zeros_like(block))
                x_ref[pl.ds(i * width, width), here] = block
                turned.append(block.T)
            turned = jnp.concatenate(turned, axis=1)
            x_ref[here, rest] = turned
            tail = dot(jnp.concatenate(halves(turned), axis=1), both)
            x_ref[here, here] = dinv_ref[k].T - h_ref[k, :, here] - tail
        else:
            x_ref[here, here] = dinv_ref[k].T - h_ref[k, :, here]
    for k in range(steps):
        for j in range(steps):

            @pl.when((info[0] == k) & (info[1] == j))
            def _():
                out_ref[...] = x_ref[pl.ds(k * width, width), pl.ds(j * width, width)]


def corner_blocks(info, live, sums, corner, dinv):
    steps, width, _ = dinv.shape
    return pl.pallas_call(
        corner_kernel,
        in_specs=[SMEM, SMEM] + [VMEM] * (len(sums) + 3),
        out_specs=VMEM,
        out_shape=jax.ShapeDtypeStruct((width, width), F32),
        scratch_shapes=[
            pltpu.VMEM((steps * width, steps * width), F32),
            pltpu.VMEM((steps, width, steps * width), F32),
        ],
        cost_estimate=pl.CostEstimate(flops=10**9, bytes_accessed=10**6, transcendentals=0),
        name="corner",
    )(info, live, *sums, *corner, dinv)


def patch_kernel(info, *refs):
    *value_refs, _, out_ref, turned_ref, sem_ref = refs
    row_blocks, cols, width, _ = out_ref.shape
    has_row, has_col, row_first, col_first = info[0], info[1], info[2], info[3]
    rows, columns = [], []
    for row_ref, even_ref, odd_ref in zip(value_refs[::3], value_refs[1::3], value_refs[2::3]):
        for c in range(row_ref.shape[1] // width):
            rows.append((row_ref, pl.ds(c * width, width)))
            columns.append((even_ref, pl.ds(c * width, width)))
            columns.append((odd_ref, pl.ds(c * width, width)))

    def row_copy(c):
        return pltpu.make_async_copy(rows[c][0].at[:, rows[c][1]], out_ref.at[0, c], sem_ref.at[c])

    def col_copy(a):
        return pltpu.make_async_copy(turned_ref.at[a], out_ref.at[a, 0], sem_ref.at[cols + a])

    @pl.when(has_row > 0)
    def _():
        for c in range(1, cols):
            row_copy(c).start()

    @pl.when(row_first > 0)
    def _():
        row_copy(0).start()

    @pl.when(has_col > 0)
    def _():
        for a in range(row_blocks):
            turned_ref[a] = columns[a][0][:, columns[a][1]].T
        for a in range(1, row_blocks):
            col_copy(a).start()
        for a in range(1, row_blocks):
            col_copy(a).wait()

    @pl.when(col_first > 0)
    def _():
        col_copy(0).start()
        col_copy(0).wait()

    @pl.when(has_row > 0)
    def _():
        for c in range(1, cols):
            row_copy(c).wait()

    @pl.when(row_first > 0)
    def _():
        row_copy(0).wait()


def patch(info, values, whole):
    row_blocks, cols, width, _ = whole.shape
    return pl.pallas_call(
        patch_kernel,
        in_specs=[SMEM] + [VMEM] * len(values) + [ANY],
        out_specs=ANY,
        out_shape=jax.ShapeDtypeStruct(whole.shape, F32),
        scratch_shapes=[pltpu.VMEM((row_blocks, width, width), F32), pltpu.SemaphoreType.DMA((row_blocks + cols,))],
        input_output_aliases={1 + len(values): 0},
        cost_estimate=pl.CostEstimate(flops=10**8, bytes_accessed=4 * 10**6, transcendentals=0),
        name="patch",
    )(info, *values, whole)


def first_kernel(info, block_ref, _, out_ref, sem_ref):
    @pl.when(info[0] > 0)
    def _():
        copy = pltpu.make_async_copy(block_ref, out_ref.at[0, 0], sem_ref)
        copy.start()
        copy.wait()


def patch_first(info, block, whole):
    return pl.pallas_call(
        first_kernel,
        in_specs=[SMEM, VMEM, ANY],
        out_specs=ANY,
        out_shape=jax.ShapeDtypeStruct(whole.shape, F32),
        scratch_shapes=[pltpu.SemaphoreType.DMA],
        input_output_aliases={2: 0},
        name="patch_first",
    )(info, block, whole)


def per_device(ainv_in, ufactor, dinv, pattern):
    row_blocks, _, cols, _, width, _ = ainv_in.shape
    steps = dinv.shape[0]
    n_row, n_col = lax.axis_size("prow"), lax.axis_size("pcol")
    blocks = ainv_in.reshape(row_blocks, cols, width, width)
    lower = ufactor.reshape(row_blocks, steps, width, width)
    p, q = lax.axis_index("prow"), lax.axis_index("pcol")
    z, y, core = p // 2, p % 2, q % 2
    n_z = n_row // 2
    row_ids = jnp.arange(row_blocks, dtype=jnp.int32) * n_row + p
    col_ids = jnp.arange(cols, dtype=jnp.int32) * n_col + q

    flags = pattern[:, :steps]
    mine = lax.dynamic_index_in_dim(flags.reshape(row_blocks, n_row, steps), p, 1, keepdims=False)
    live = ((mine > 0) & (row_ids >= steps)[:, None]).astype(jnp.int32)
    live_corner = flags[:steps]
    mine = lax.dynamic_index_in_dim(flags.reshape(cols, n_col, steps), q, 1, keepdims=False)
    live_cols = ((mine > 0) & (col_ids >= steps)[:, None]).astype(jnp.int32)
    row_live = lax.dynamic_index_in_dim(live_cols, jnp.minimum(p, steps - 1), 1, keepdims=False) > 0

    def at(zz, yy):
        return zz % n_z * 2 + yy

    flip_y = [(d, d ^ 1) for d in range(n_row)]
    flip_z = [(d, d ^ 2) for d in range(n_row)]
    mirror = [(d, at(n_z - 1 - d // 2, d % 2)) for d in range(n_row)]
    flip_core = [(d, d ^ 1) for d in range(n_col)]

    half = width // 2
    mine = lax.dynamic_slice_in_dim(lower[0], core * half, half, axis=1)

    def join(bit, own, other):
        return jnp.where(bit == 0, jnp.concatenate([own, other]), jnp.concatenate([other, own]))

    def ring(shift):
        return [(at(zz, yy), at(zz + shift, yy)) for zz in range(n_z) for yy in range(2)]

    pair = join(y, mine[None], lax.ppermute(mine[None], "prow", flip_y))
    moved = [pair] + [lax.ppermute(pair, "prow", ring(shift)) for shift in (1, 2, 3)]
    corner = []
    for t in range(steps // 2):
        away = (z - t) % n_z
        corner.append(jnp.where(away == 0, moved[0], jnp.where(away == 1, moved[1], jnp.where(away == 2, moved[2], moved[3]))))
    corner = jnp.concatenate(corner)
    corner = corner, lax.ppermute(corner, "pcol", flip_core)

    n_dest = steps // 2

    both, grid = ("prow", "pcol"), [(x, h, c) for x in range(n_col // 4) for h in range(2) for c in range(2)]

    def device(x, h, c, zz, yy):
        return at(zz, yy) * n_col + x * 4 + h * 2 + c

    whole, parts = None, []
    for first, count in PARTS:
        whole, part = products(blocks, lower, live, whole, first, count)
        parts.append(part)

    def near(shift):
        return [(s, d) for s, d in ring(shift) if d < steps]

    def slot(zz, par):
        return jnp.minimum(zz % n_z, n_dest - 1) * 2 + par

    take = [slot(z + 2, 0), slot(z + 1, 1), slot(z + 2, 1), slot(z - 1, 0)]
    take += [slot(z + 1, 0), slot(z - 1, 1), slot(z, 0), slot(z, 1), core]
    up, down, up2, down2, own = eliminate(parts, corner, live_corner, jnp.stack(take).astype(jnp.int32))
    up = lax.ppermute(up, "prow", ring(1))
    down = lax.ppermute(down, "prow", ring(-1))
    up2 = lax.ppermute(up2 + up[0], "prow", near(1))
    down2 = lax.ppermute(down2 + down[0], "prow", near(-1))
    even, odd = own[0] + down[1] + up2, own[1] + up[1] + down2
    keep, give = jnp.where(y == 0, even, odd), jnp.where(y == 0, odd, even)
    full = keep + lax.ppermute(give, "prow", [(d, d ^ 1) for d in range(steps)])
    mask = jnp.broadcast_to(row_live[:, None], (cols, width)).reshape(1, cols * width)
    row = jnp.where(mask, full, jnp.zeros_like(full))

    def turn(k, x, h, c):
        return at(k // 2, k % 2) * n_col + x * 4 + h * 2 + c, device(x, k // 2 % 2, k % 2, x % 2 * 2 + h, c)

    places = [(h, c, zz, yy) for h in range(2) for c in range(2) for zz in range(n_z) for yy in range(2)]

    def slide(place, start, end):
        h, c, zz, yy = place
        return device(start, h, c, zz, yy), device(end, h, c, zz, yy)

    x = q // 4
    first = lax.ppermute(row, both, [turn(k, *place) for k in range(4) for place in grid])
    second = lax.ppermute(row, both, [turn(k, *place) for k in range(4, steps) for place in grid])
    odd0 = lax.ppermute(first, both, [slide(pl_, pl_[2] // 2 + 2, 0) for pl_ in places])
    odd1 = lax.ppermute(second, both, [slide(pl_, pl_[2] // 2 + 2, 1) for pl_ in places if pl_[0] == 0])
    route = [slide(pl_, 0, 1) for pl_ in places if pl_[2] // 2 == 0 and pl_[0] == 0]
    route += [slide(pl_, 1, 0) for pl_ in places if pl_[2] // 2 == 1]
    moved = lax.ppermute(jnp.where(x == 0, second, first), both, route)
    mine = jnp.where(x == 0, first, second)
    values = [row, jnp.where(x == z // 2, mine, moved), jnp.where(x == 0, odd0, odd1)]

    sums = column_products(values[1:], lower, live)

    def here(perm):
        return [(s * n_col + d, t * n_col + d) for s, t in perm for d in range(steps)]

    for perm in (flip_y, flip_z, mirror):
        sums = sums + lax.ppermute(sums, both, here(perm))
    turns = [lax.ppermute(sums, "pcol", [(d, (d + t) % steps) for d in range(steps)]) for t in (2, 4)]
    sums = [sums, *turns]
    sums += [lax.ppermute(v, "pcol", [(d, d ^ 1) for d in range(steps)]) for v in sums]
    slots = [(q + steps - t) % steps for t in (0, 2, 4)]
    slots += [s ^ 1 for s in slots]

    has_row, has_col = p < steps, q < steps
    info = jnp.stack([has_row, has_col, has_row & ~has_col, has_col & ~has_row]).astype(jnp.int32)
    whole = patch(info, values, whole)
    info = jnp.stack([p, q, core, *slots]).astype(jnp.int32)
    block = corner_blocks(info, live_corner, sums, corner, dinv)
    info = jnp.stack([has_row & has_col]).astype(jnp.int32)
    whole = patch_first(info, block, whole)
    return whole.reshape(ainv_in.shape)


def solution(mesh):
    placed = (
        P(None, "prow", None, "pcol", None, None),
        P(None, "prow", None, None, None),
        P(),
        P(),
    )
    return jax.shard_map(
        per_device,
        mesh=mesh,
        in_specs=placed,
        out_specs=P(None, "prow", None, "pcol", None, None),
        check_vma=False,
    )
```

```python
import jax
import jax.numpy as jnp
from jax import lax
from jax.experimental import pallas as pl
from jax.experimental.pallas import tpu as pltpu
from jax.sharding import PartitionSpec as P


F32, BF16 = jnp.float32, jnp.bfloat16
PARTS = ((0, 8), (8, 10))
SIZES = (3, 4, 4)
VMEM = pl.BlockSpec(memory_space=pltpu.VMEM)
SMEM = pl.BlockSpec(memory_space=pltpu.SMEM)
ANY = pl.BlockSpec(memory_space=pl.ANY)


def halves(value):
    high = value.astype(BF16)
    return high, (value - high.astype(F32)).astype(BF16)


def stacked(core, own, other):
    return jnp.concatenate([jnp.where(core > 0, other, own), jnp.where(core > 0, own, other)], axis=0)


def dot(left, right):
    return jnp.dot(left, right, preferred_element_type=F32)


def product_kernel(live, x_ref, u_ref, *refs):
    copy_ref, out_ref = refs[-2:]
    step = pl.program_id(0)
    rows, cols, _, _ = x_ref.shape
    steps = u_ref.shape[1]
    left, high, low = [], [], []
    for r in range(rows):
        wide = []
        for k in range(steps):
            block = u_ref[r, k]
            wide.append(jnp.where(live[step * rows + r, k] > 0, block, jnp.zeros_like(block)))
        left.append(jnp.concatenate(wide, axis=1))
        value = jnp.concatenate([x_ref[r, c] for c in range(cols)], axis=1)
        for c in range(cols):
            copy_ref[r, c] = x_ref[r, c]
        a, b = halves(value)
        high.append(a)
        low.append(b)
    left = jnp.concatenate(left, axis=0).T
    both = jnp.concatenate([left, left], axis=1)
    term = dot(both, jnp.concatenate(high + low, axis=0))
    term = term.reshape(out_ref.shape)

    @pl.when(step == 0)
    def _():
        out_ref[...] = term

    @pl.when(step > 0)
    def _():
        out_ref[...] += term


def products(blocks, lower, live, whole, first, count, rows=2):
    _, cols, width, _ = blocks.shape
    steps = lower.shape[1]
    start = first // rows
    known = [] if whole is None else [whole]
    return pl.pallas_call(
        product_kernel,
        grid_spec=pltpu.PrefetchScalarGridSpec(
            num_scalar_prefetch=1,
            grid=(count // rows,),
            in_specs=[
                pl.BlockSpec((rows, cols, width, width), lambda i, _: (start + i, 0, 0, 0)),
                pl.BlockSpec((rows, steps, width, width), lambda i, _: (start + i, 0, 0, 0)),
            ]
            + [ANY] * len(known),
            out_specs=[
                pl.BlockSpec((rows, cols, width, width), lambda i, _: (start + i, 0, 0, 0)),
                pl.BlockSpec((steps, width, cols * width), lambda i, _: (0, 0, 0)),
            ],
        ),
        out_shape=[
            jax.ShapeDtypeStruct(blocks.shape, F32),
            jax.ShapeDtypeStruct((steps, width, cols * width), F32),
        ],
        input_output_aliases={3: 0} if known else {},
        cost_estimate=pl.CostEstimate(
            flops=4 * count * cols * steps * width**3, bytes_accessed=8 * count * cols * width**2, transcendentals=0
        ),
        name="products",
    )(live[first : first + count], blocks, lower, *known)


def eliminate_kernel(take, live, *refs):
    *part_refs, u_ref, v_ref = refs[: -2 * len(SIZES) - 1]
    places, w_ref = refs[-2 * len(SIZES) - 1 : -1], refs[-1]
    steps = w_ref.shape[0]
    high, low = [], []
    for k in reversed(range(steps)):
        total = part_refs[0][k]
        for ref in part_refs[1:]:
            total = total + ref[k]
        if high:
            blocks = []
            for j in range(k + 1, steps):
                block = stacked(take[0], u_ref[j, k], v_ref[j, k])
                blocks.append(jnp.where(live[j, k] > 0, block, jnp.zeros_like(block)).T)
            left = jnp.concatenate(blocks + blocks, axis=1)
            total = total + dot(left, jnp.concatenate(high[::-1] + low[::-1], axis=0))
        total = -total
        w_ref[k] = total
        a, b = halves(total)
        high.append(a)
        low.append(b)
    at = 1
    for n, ref in enumerate(places):
        count, _, wide = ref.shape
        for m in range(count):
            ref[m] = w_ref[take[at], :, pl.ds(n // 2 * wide, wide)]
            at += 1


def eliminate(parts, corner, live, take):
    _, width, wide = parts[0].shape
    shapes = [jax.ShapeDtypeStruct((n, width, wide // len(SIZES)), F32) for n in SIZES for _ in range(2)]
    return pl.pallas_call(
        eliminate_kernel,
        in_specs=[SMEM, SMEM] + [VMEM] * (len(parts) + 2),
        out_specs=[VMEM] * len(shapes),
        out_shape=shapes,
        scratch_shapes=[pltpu.VMEM(parts[0].shape, F32)],
        cost_estimate=pl.CostEstimate(flops=1000 * parts[0].size, bytes_accessed=20 * parts[0].size, transcendentals=0),
        name="eliminate",
    )(take, live, *parts, *corner)


def halving_kernel(take, *refs):
    given, places = refs[: len(refs) // 2], refs[len(refs) // 2 :]
    at = 0
    for n, ref in enumerate(places):
        stay_ref, came_ref = given[n // 2 * 2], given[n // 2 * 2 + 1]
        for m in range(ref.shape[0]):
            ref[m] = stay_ref[take[at]] + came_ref[take[at]]
            at += 1


def halving(take, count, given):
    _, width, wide = given[0].shape
    shapes = [jax.ShapeDtypeStruct((count, width, wide), F32)] * len(given)
    return pl.pallas_call(
        halving_kernel,
        in_specs=[SMEM] + [VMEM] * len(given),
        out_specs=[VMEM] * len(given),
        out_shape=shapes,
        cost_estimate=pl.CostEstimate(flops=10**8, bytes_accessed=16 * width * wide * len(given), transcendentals=0),
        name="halving",
    )(take, *given)


def row_kernel(live, *refs):
    *given, row_ref = refs
    width = row_ref.shape[0]
    count = given[0].shape[2] // width
    for n in range(row_ref.shape[1] // width):
        part = pl.ds(n % count * width, width)
        value = given[n // count * 2][0, :, part] + given[n // count * 2 + 1][0, :, part]
        row_ref[:, pl.ds(n * width, width)] = jnp.where(live[n] > 0, value, jnp.zeros_like(value))


def masked_row(live, given):
    _, width, wide = given[0].shape
    return pl.pallas_call(
        row_kernel,
        in_specs=[SMEM] + [VMEM] * len(given),
        out_specs=VMEM,
        out_shape=jax.ShapeDtypeStruct((width, wide * len(given) // 2), F32),
        cost_estimate=pl.CostEstimate(flops=10**7, bytes_accessed=8 * width * wide * len(given), transcendentals=0),
        name="row",
    )(live, *given)


def column_kernel(live, *refs):
    *value_refs, u_ref, upper_ref, lower_ref = refs
    _, steps, width, _ = u_ref.shape
    total, a = None, 0
    for even_ref, odd_ref in zip(value_refs[::2], value_refs[1::2]):
        for c in range(even_ref.shape[1] // width):
            part = pl.ds(c * width, width)
            value = jnp.concatenate([even_ref[:, part], odd_ref[:, part]], axis=1)
            left = jnp.concatenate(halves(value), axis=0)
            right = []
            for r in (a, a + 1):
                wide = []
                for k in range(steps):
                    block = u_ref[r, k]
                    wide.append(jnp.where(live[r, k] > 0, block, jnp.zeros_like(block)))
                right.append(jnp.concatenate(wide, axis=1))
            term = dot(left, jnp.concatenate(right, axis=0))
            total = term if total is None else total + term
            a += 2
    total = total[:width] + total[width:]
    upper_ref[...] = total[: width // 2]
    lower_ref[...] = total[width // 2 :]


def column_products(values, lower, live):
    row_blocks, steps, width, _ = lower.shape
    return pl.pallas_call(
        column_kernel,
        in_specs=[SMEM] + [VMEM] * (len(values) + 1),
        out_specs=[VMEM] * 2,
        out_shape=[jax.ShapeDtypeStruct((width // 2, steps * width), F32)] * 2,
        cost_estimate=pl.CostEstimate(flops=4 * row_blocks * steps * width**3, bytes_accessed=6 * 10**6, transcendentals=0),
        name="column",
    )(live, *values, lower)


def corner_kernel(info, live, *refs):
    *sum_refs, u_ref, v_ref, dinv_ref, out_ref, x_ref, h_ref = refs
    steps, width, _ = dinv_ref.shape
    for n, ref in enumerate(sum_refs):
        h_ref[info[3 + n]] = ref[...]
    for k in reversed(range(steps)):
        here = pl.ds(k * width, width)
        later = steps - 1 - k
        if later:
            right = []
            for j in range(k + 1, steps):
                block = stacked(info[2], u_ref[j, k], v_ref[j, k])
                right.append(jnp.where(live[j, k] > 0, block, jnp.zeros_like(block)))
            right = jnp.concatenate(right, axis=0)
            both = jnp.concatenate([right, right], axis=0)
            rest = pl.ds((k + 1) * width, later * width)
            known = jnp.concatenate(halves(x_ref[rest, rest]), axis=1)
            value = dot(known, both)
            turned = []
            for i in range(k + 1, steps):
                at = (i - k - 1) * width
                block = -(value[at : at + width] + h_ref[i, :, here])
                block = jnp.where(live[i, k] > 0, block, jnp.zeros_like(block))
                x_ref[pl.ds(i * width, width), here] = block
                turned.append(block.T)
            turned = jnp.concatenate(turned, axis=1)
            x_ref[here, rest] = turned
            tail = dot(jnp.concatenate(halves(turned), axis=1), both)
            x_ref[here, here] = dinv_ref[k].T - h_ref[k, :, here] - tail
        else:
            x_ref[here, here] = dinv_ref[k].T - h_ref[k, :, here]
    for k in range(steps):
        for j in range(steps):

            @pl.when((info[0] == k) & (info[1] == j))
            def _():
                out_ref[...] = x_ref[pl.ds(k * width, width), pl.ds(j * width, width)]


def corner_blocks(info, live, sums, corner, dinv):
    steps, width, _ = dinv.shape
    return pl.pallas_call(
        corner_kernel,
        in_specs=[SMEM, SMEM] + [VMEM] * (len(sums) + 3),
        out_specs=VMEM,
        out_shape=jax.ShapeDtypeStruct((width, width), F32),
        scratch_shapes=[
            pltpu.VMEM((steps * width, steps * width), F32),
            pltpu.VMEM((steps, width, steps * width), F32),
        ],
        cost_estimate=pl.CostEstimate(flops=10**9, bytes_accessed=10**6, transcendentals=0),
        name="corner",
    )(info, live, *sums, *corner, dinv)


def patch_kernel(info, *refs):
    *value_refs, _, out_ref, turned_ref, sem_ref = refs
    row_blocks, cols, width, _ = out_ref.shape
    has_row, has_col, row_first, col_first = info[0], info[1], info[2], info[3]
    rows, columns = [], []
    for row_ref, even_ref, odd_ref in zip(value_refs[::3], value_refs[1::3], value_refs[2::3]):
        for c in range(row_ref.shape[1] // width):
            rows.append((row_ref, pl.ds(c * width, width)))
            columns.append((even_ref, pl.ds(c * width, width)))
            columns.append((odd_ref, pl.ds(c * width, width)))

    def row_copy(c):
        return pltpu.make_async_copy(rows[c][0].at[:, rows[c][1]], out_ref.at[0, c], sem_ref.at[c])

    def col_copy(a):
        return pltpu.make_async_copy(turned_ref.at[a], out_ref.at[a, 0], sem_ref.at[cols + a])

    @pl.when(has_row > 0)
    def _():
        for c in range(1, cols):
            row_copy(c).start()

    @pl.when(row_first > 0)
    def _():
        row_copy(0).start()

    @pl.when(has_col > 0)
    def _():
        for a in range(row_blocks):
            turned_ref[a] = columns[a][0][:, columns[a][1]].T
        for a in range(1, row_blocks):
            col_copy(a).start()
        for a in range(1, row_blocks):
            col_copy(a).wait()

    @pl.when(col_first > 0)
    def _():
        col_copy(0).start()
        col_copy(0).wait()

    @pl.when(has_row > 0)
    def _():
        for c in range(1, cols):
            row_copy(c).wait()

    @pl.when(row_first > 0)
    def _():
        row_copy(0).wait()


def patch(info, values, whole):
    row_blocks, cols, width, _ = whole.shape
    return pl.pallas_call(
        patch_kernel,
        in_specs=[SMEM] + [VMEM] * len(values) + [ANY],
        out_specs=ANY,
        out_shape=jax.ShapeDtypeStruct(whole.shape, F32),
        scratch_shapes=[pltpu.VMEM((row_blocks, width, width), F32), pltpu.SemaphoreType.DMA((row_blocks + cols,))],
        input_output_aliases={1 + len(values): 0},
        cost_estimate=pl.CostEstimate(flops=10**8, bytes_accessed=4 * 10**6, transcendentals=0),
        name="patch",
    )(info, *values, whole)


def first_kernel(info, block_ref, _, out_ref, sem_ref):
    @pl.when(info[0] > 0)
    def _():
        copy = pltpu.make_async_copy(block_ref, out_ref.at[0, 0], sem_ref)
        copy.start()
        copy.wait()


def patch_first(info, block, whole):
    return pl.pallas_call(
        first_kernel,
        in_specs=[SMEM, VMEM, ANY],
        out_specs=ANY,
        out_shape=jax.ShapeDtypeStruct(whole.shape, F32),
        scratch_shapes=[pltpu.SemaphoreType.DMA],
        input_output_aliases={2: 0},
        name="patch_first",
    )(info, block, whole)


def per_device(ainv_in, ufactor, dinv, pattern):
    row_blocks, _, cols, _, width, _ = ainv_in.shape
    steps = dinv.shape[0]
    n_row, n_col = lax.axis_size("prow"), lax.axis_size("pcol")
    blocks = ainv_in.reshape(row_blocks, cols, width, width)
    lower = ufactor.reshape(row_blocks, steps, width, width)
    p, q = lax.axis_index("prow"), lax.axis_index("pcol")
    z, y, core = p // 2, p % 2, q % 2
    n_z = n_row // 2
    row_ids = jnp.arange(row_blocks, dtype=jnp.int32) * n_row + p
    col_ids = jnp.arange(cols, dtype=jnp.int32) * n_col + q

    flags = pattern[:, :steps]
    mine = lax.dynamic_index_in_dim(flags.reshape(row_blocks, n_row, steps), p, 1, keepdims=False)
    live = ((mine > 0) & (row_ids >= steps)[:, None]).astype(jnp.int32)
    live_corner = flags[:steps]
    mine = lax.dynamic_index_in_dim(flags.reshape(cols, n_col, steps), q, 1, keepdims=False)
    live_cols = ((mine > 0) & (col_ids >= steps)[:, None]).astype(jnp.int32)
    row_live = lax.dynamic_index_in_dim(live_cols, jnp.minimum(p, steps - 1), 1, keepdims=False) > 0

    def at(zz, yy):
        return zz % n_z * 2 + yy

    flip_y = [(d, d ^ 1) for d in range(n_row)]
    flip_z = [(d, d ^ 2) for d in range(n_row)]
    mirror = [(d, at(n_z - 1 - d // 2, d % 2)) for d in range(n_row)]
    flip_core = [(d, d ^ 1) for d in range(n_col)]

    half = width // 2
    mine = lax.dynamic_slice_in_dim(lower[0], core * half, half, axis=1)

    def join(bit, own, other):
        return jnp.where(bit == 0, jnp.concatenate([own, other]), jnp.concatenate([other, own]))

    def ring(shift):
        return [(at(zz, yy), at(zz + shift, yy)) for zz in range(n_z) for yy in range(2)]

    pair = join(y, mine[None], lax.ppermute(mine[None], "prow", flip_y))
    moved = [pair] + [lax.ppermute(pair, "prow", ring(shift)) for shift in (1, 2, 3)]
    corner = []
    for t in range(steps // 2):
        away = (z - t) % n_z
        corner.append(jnp.where(away == 0, moved[0], jnp.where(away == 1, moved[1], jnp.where(away == 2, moved[2], moved[3]))))
    corner = jnp.concatenate(corner)
    corner = corner, lax.ppermute(corner, "pcol", flip_core)

    both, grid = ("prow", "pcol"), [(x, h, c) for x in range(n_col // 4) for h in range(2) for c in range(2)]

    def device(x, h, c, zz, yy):
        return at(zz, yy) * n_col + x * 4 + h * 2 + c

    whole, parts = None, []
    for first, count in PARTS:
        whole, part = products(blocks, lower, live, whole, first, count)
        parts.append(part)

    outer, low = (z == 0) | (z == n_z - 1), z < 2
    mine, other = y, 1 - y

    def table(*rows):
        return jnp.stack([jnp.asarray(v, jnp.int32) for row in rows for v in row])

    def either(flag, yes, no):
        return [jnp.where(flag, a, b) for a, b in zip(yes, no)]

    ends, middle = (0, 1, 0, 0), (2, 3, 4, 5)
    front, back = (0, 1, 2, 3), (4, 5, 0, 0)
    take = table(
        [core],
        [other, 2 + other, 4 + other],
        [mine, 2 + mine, 4 + mine],
        either(outer, middle, ends),
        either(outer, ends, middle),
        either(low, back, front),
        either(low, front, back),
    )
    send_a, keep_a, send_b, keep_b, send_c, keep_c = eliminate(parts, corner, live_corner, take)
    over_m = [(s, d) for s, d in mirror if d < steps]
    came_a = lax.ppermute(send_a, "prow", flip_y)
    came_b = lax.ppermute(send_b, "prow", flip_z)
    came_c = lax.ppermute(send_c, "prow", mirror)
    take = table(
        either(outer, (1, 2), (0, 0)),
        either(outer, (0, 0), (1, 2)),
        either(z == 1, (2, 3), (0, 1)),
        either(z == 2, (2, 3), (0, 1)),
        either(low, (other, 2 + other), (other, other)),
        either(low, (mine, 2 + mine), (mine, mine)),
    )
    given = [keep_a, came_a, keep_b, came_b, keep_c, came_c]
    send_a, keep_a, send_b, keep_b, send_c, keep_c = halving(take, 2, given)
    came_a = lax.ppermute(send_a, "prow", flip_z)
    came_b = lax.ppermute(send_b, "prow", over_m)
    came_c = lax.ppermute(send_c, "prow", flip_y)
    take = table(
        [jnp.where(z == 1, 1, 0), jnp.where(z == 2, 1, 0), other, mine, jnp.where(z == 0, 1, 0), jnp.where(z == 1, 1, 0)]
    )
    given = [keep_a, came_a, keep_b, came_b, keep_c, came_c]
    send_a, keep_a, send_b, keep_b, send_c, keep_c = halving(take, 1, given)
    came_a = lax.ppermute(send_a, "prow", over_m)
    came_b = lax.ppermute(send_b, "prow", [(s, d) for s, d in flip_y if d < steps])
    came_c = lax.ppermute(send_c, "prow", [(s, d) for s, d in flip_z if d < steps])
    row = masked_row(row_live.astype(jnp.int32), [keep_a, came_a, keep_b, came_b, keep_c, came_c])

    def turn(k, x, h, c):
        return at(k // 2, k % 2) * n_col + x * 4 + h * 2 + c, device(x, k // 2 % 2, k % 2, x % 2 * 2 + h, c)

    places = [(h, c, zz, yy) for h in range(2) for c in range(2) for zz in range(n_z) for yy in range(2)]

    def slide(place, start, end):
        h, c, zz, yy = place
        return device(start, h, c, zz, yy), device(end, h, c, zz, yy)

    x = q // 4
    first = lax.ppermute(row, both, [turn(k, *place) for k in range(4) for place in grid])
    second = lax.ppermute(row, both, [turn(k, *place) for k in range(4, steps) for place in grid])
    odd0 = lax.ppermute(first, both, [slide(pl_, pl_[2] // 2 + 2, 0) for pl_ in places])
    odd1 = lax.ppermute(second, both, [slide(pl_, pl_[2] // 2 + 2, 1) for pl_ in places if pl_[0] == 0])
    route = [slide(pl_, 0, 1) for pl_ in places if pl_[2] // 2 == 0 and pl_[0] == 0]
    route += [slide(pl_, 1, 0) for pl_ in places if pl_[2] // 2 == 1]
    moved = lax.ppermute(jnp.where(x == 0, second, first), both, route)
    mine = jnp.where(x == 0, first, second)
    values = [row, jnp.where(x == z // 2, mine, moved), jnp.where(x == 0, odd0, odd1)]

    upper, under = column_products(values[1:], lower, live)

    def here(perm):
        return [(s * n_col + d, t * n_col + d) for s, t in perm for d in range(steps)]

    orders = (flip_y, flip_z), (flip_z, mirror), (mirror, flip_y)
    for (one, two) in orders:
        came = lax.ppermute(upper, both, here(one)), lax.ppermute(under, both, here(two))
        upper, under = upper + came[0], under + came[1]
    sums = jnp.concatenate([upper, under])

    def around(t):
        route = []
        for d in range(steps):
            to = (d + t) % steps
            flip = d // 2 % 2 ^ to // 2 % 2
            route += [(s * n_col + d, (s ^ flip) * n_col + to) for s in range(n_row)]
        return route

    turns = [lax.ppermute(sums, both, around(t)) for t in (2, 4)]
    sums = [sums, *turns]
    sums += [lax.ppermute(v, "pcol", [(d, d ^ 1) for d in range(steps)]) for v in sums]
    slots = [(q + steps - t) % steps for t in (0, 2, 4)]
    slots += [s ^ 1 for s in slots]

    has_row, has_col = p < steps, q < steps
    info = jnp.stack([has_row, has_col, has_row & ~has_col, has_col & ~has_row]).astype(jnp.int32)
    whole = patch(info, values, whole)
    info = jnp.stack([p, q, core, *slots]).astype(jnp.int32)
    block = corner_blocks(info, live_corner, sums, corner, dinv)
    info = jnp.stack([has_row & has_col]).astype(jnp.int32)
    whole = patch_first(info, block, whole)
    return whole.reshape(ainv_in.shape)


def solution(mesh):
    placed = (
        P(None, "prow", None, "pcol", None, None),
        P(None, "prow", None, None, None),
        P(),
        P(),
    )
    return jax.shard_map(
        per_device,
        mesh=mesh,
        in_specs=placed,
        out_specs=P(None, "prow", None, "pcol", None, None),
        check_vma=False,
    )
```

```python
import functools

import jax
import jax.numpy as jnp
from jax import lax
from jax.experimental import pallas as pl
from jax.experimental.pallas import tpu as pltpu
from jax.sharding import PartitionSpec as P


F32, BF16 = jnp.float32, jnp.bfloat16
PARTS = ((0, 8), (8, 10))
SIZES = (3, 4, 4)
CORNER, COLS, IDS = 18, 24, 33
VMEM = pl.BlockSpec(memory_space=pltpu.VMEM)
SMEM = pl.BlockSpec(memory_space=pltpu.SMEM)
ANY = pl.BlockSpec(memory_space=pl.ANY)


def halves(value):
    high = value.astype(BF16)
    return high, (value - high.astype(F32)).astype(BF16)


def stacked(core, own, other):
    return jnp.concatenate([jnp.where(core > 0, other, own), jnp.where(core > 0, own, other)], axis=0)


def dot(left, right):
    return jnp.dot(left, right, preferred_element_type=F32)


def product_kernel(start, masks, x_ref, u_ref, *refs):
    copy_ref, out_ref = refs[-2:]
    step = pl.program_id(0)
    rows, cols, _, _ = x_ref.shape
    steps = u_ref.shape[1]
    left, high, low = [], [], []
    for r in range(rows):
        wide = []
        for k in range(steps):
            block = u_ref[r, k]
            wide.append(jnp.where(masks[start + step * rows + r, k] > 0, block, jnp.zeros_like(block)))
        left.append(jnp.concatenate(wide, axis=1))
        value = jnp.concatenate([x_ref[r, c] for c in range(cols)], axis=1)
        for c in range(cols):
            copy_ref[r, c] = x_ref[r, c]
        a, b = halves(value)
        high.append(a)
        low.append(b)
    left = jnp.concatenate(left, axis=0).T
    both = jnp.concatenate([left, left], axis=1)
    term = dot(both, jnp.concatenate(high + low, axis=0))
    term = term.reshape(out_ref.shape)

    @pl.when(step == 0)
    def _():
        out_ref[...] = term

    @pl.when(step > 0)
    def _():
        out_ref[...] += term


def products(blocks, lower, masks, whole, first, count, rows=2):
    _, cols, width, _ = blocks.shape
    steps = lower.shape[1]
    start = first // rows
    known = [] if whole is None else [whole]
    return pl.pallas_call(
        functools.partial(product_kernel, first),
        grid_spec=pltpu.PrefetchScalarGridSpec(
            num_scalar_prefetch=1,
            grid=(count // rows,),
            in_specs=[
                pl.BlockSpec((rows, cols, width, width), lambda i, _: (start + i, 0, 0, 0)),
                pl.BlockSpec((rows, steps, width, width), lambda i, _: (start + i, 0, 0, 0)),
            ]
            + [ANY] * len(known),
            out_specs=[
                pl.BlockSpec((rows, cols, width, width), lambda i, _: (start + i, 0, 0, 0)),
                pl.BlockSpec((steps, width, cols * width), lambda i, _: (0, 0, 0)),
            ],
        ),
        out_shape=[
            jax.ShapeDtypeStruct(blocks.shape, F32),
            jax.ShapeDtypeStruct((steps, width, cols * width), F32),
        ],
        input_output_aliases={3: 0} if known else {},
        cost_estimate=pl.CostEstimate(
            flops=4 * count * cols * steps * width**3, bytes_accessed=8 * count * cols * width**2, transcendentals=0
        ),
        name="products",
    )(masks, blocks, lower, *known)


def first_pieces(z, y):
    outer, low, other = (z == 0) | (z == 3), z < 2, 1 - y

    def either(flag, yes, no):
        return [jnp.where(flag, a, b) for a, b in zip(yes, no)]

    ends, middle = (0, 1, 0, 0), (2, 3, 4, 5)
    front, back = (0, 1, 2, 3), (4, 5, 0, 0)
    return [
        [other, 2 + other, 4 + other],
        [y, 2 + y, 4 + y],
        either(outer, middle, ends),
        either(outer, ends, middle),
        either(low, back, front),
        either(low, front, back),
    ]


def later_pieces(group, stage, z, y):
    outer, low, other = (z == 0) | (z == 3), z < 2, 1 - y
    one, two = jnp.where(z == 1, 1, 0), jnp.where(z == 2, 1, 0)
    if stage == 2:
        return [
            ([jnp.where(outer, 1, 0), jnp.where(outer, 2, 0)], [jnp.where(outer, 0, 1), jnp.where(outer, 0, 2)]),
            ([2 * one, 2 * one + 1], [2 * two, 2 * two + 1]),
            ([other, jnp.where(low, 2 + other, other)], [y, jnp.where(low, 2 + y, y)]),
        ][group]
    return [([one], [two]), ([other], [y]), ([jnp.where(z == 0, 1, 0)], [one])][group]


def place_of(masks):
    p, q = masks[IDS, 0], masks[IDS, 1]
    return p, q, p // 2, p % 2


def eliminate_kernel(masks, *refs):
    *part_refs, u_ref, v_ref = refs[: -2 * len(SIZES) - 1]
    places, w_ref = refs[-2 * len(SIZES) - 1 : -1], refs[-1]
    steps = w_ref.shape[0]
    _, q, z, y = place_of(masks)
    high, low = [], []
    for k in reversed(range(steps)):
        total = part_refs[0][k]
        for ref in part_refs[1:]:
            total = total + ref[k]
        if high:
            blocks = []
            for j in range(k + 1, steps):
                block = stacked(q % 2, u_ref[j, k], v_ref[j, k])
                blocks.append(jnp.where(masks[CORNER + j, k] > 0, block, jnp.zeros_like(block)).T)
            left = jnp.concatenate(blocks + blocks, axis=1)
            total = total + dot(left, jnp.concatenate(high[::-1] + low[::-1], axis=0))
        total = -total
        w_ref[k] = total
        a, b = halves(total)
        high.append(a)
        low.append(b)
    for n, (ref, pieces) in enumerate(zip(places, first_pieces(z, y))):
        for m, k in enumerate(pieces):
            ref[m] = w_ref[k, :, pl.ds(n // 2 * ref.shape[2], ref.shape[2])]


def eliminate(masks, parts, corner):
    _, width, wide = parts[0].shape
    shapes = [jax.ShapeDtypeStruct((n, width, wide // len(SIZES)), F32) for n in SIZES for _ in range(2)]
    return pl.pallas_call(
        eliminate_kernel,
        in_specs=[SMEM] + [VMEM] * (len(parts) + 2),
        out_specs=[VMEM] * len(shapes),
        out_shape=shapes,
        scratch_shapes=[pltpu.VMEM(parts[0].shape, F32)],
        cost_estimate=pl.CostEstimate(flops=1000 * parts[0].size, bytes_accessed=20 * parts[0].size, transcendentals=0),
        name="eliminate",
    )(masks, *parts, *corner)


def halving_kernel(group, stage, masks, stay_ref, came_ref, send_ref, keep_ref):
    _, _, z, y = place_of(masks)
    for ref, pieces in zip((send_ref, keep_ref), later_pieces(group, stage, z, y)):
        for m, n in enumerate(pieces):
            ref[m] = stay_ref[n] + came_ref[n]


def halving(masks, group, stage, stay, came):
    _, width, wide = stay.shape
    return pl.pallas_call(
        functools.partial(halving_kernel, group, stage),
        in_specs=[SMEM, VMEM, VMEM],
        out_specs=[VMEM] * 2,
        out_shape=[jax.ShapeDtypeStruct((4 - stage, width, wide), F32)] * 2,
        cost_estimate=pl.CostEstimate(flops=10**8, bytes_accessed=32 * width * wide, transcendentals=0),
        name="halving",
    )(masks, stay, came)


def row_kernel(masks, *refs):
    *given, row_ref = refs
    width = row_ref.shape[0]
    count = given[0].shape[2] // width
    p, _, _, _ = place_of(masks)
    k = jnp.minimum(p, COLS - CORNER - 1)
    for n in range(row_ref.shape[1] // width):
        part = pl.ds(n % count * width, width)
        value = given[n // count * 2][0, :, part] + given[n // count * 2 + 1][0, :, part]
        row_ref[:, pl.ds(n * width, width)] = jnp.where(masks[COLS + n, k] > 0, value, jnp.zeros_like(value))


def masked_row(masks, given):
    _, width, wide = given[0].shape
    return pl.pallas_call(
        row_kernel,
        in_specs=[SMEM] + [VMEM] * len(given),
        out_specs=VMEM,
        out_shape=jax.ShapeDtypeStruct((width, wide * len(given) // 2), F32),
        cost_estimate=pl.CostEstimate(flops=10**7, bytes_accessed=8 * width * wide * len(given), transcendentals=0),
        name="row",
    )(masks, *given)


def column_kernel(masks, *refs):
    *value_refs, u_ref, upper_ref, lower_ref = refs
    _, steps, width, _ = u_ref.shape
    total, a = None, 0
    for even_ref, odd_ref in zip(value_refs[::2], value_refs[1::2]):
        for c in range(even_ref.shape[1] // width):
            part = pl.ds(c * width, width)
            value = jnp.concatenate([even_ref[:, part], odd_ref[:, part]], axis=1)
            left = jnp.concatenate(halves(value), axis=0)
            right = []
            for r in (a, a + 1):
                wide = []
                for k in range(steps):
                    block = u_ref[r, k]
                    wide.append(jnp.where(masks[r, k] > 0, block, jnp.zeros_like(block)))
                right.append(jnp.concatenate(wide, axis=1))
            term = dot(left, jnp.concatenate(right, axis=0))
            total = term if total is None else total + term
            a += 2
    total = total[:width] + total[width:]
    upper_ref[...] = total[: width // 2]
    lower_ref[...] = total[width // 2 :]


def column_products(values, lower, masks):
    row_blocks, steps, width, _ = lower.shape
    return pl.pallas_call(
        column_kernel,
        in_specs=[SMEM] + [VMEM] * (len(values) + 1),
        out_specs=[VMEM] * 2,
        out_shape=[jax.ShapeDtypeStruct((width // 2, steps * width), F32)] * 2,
        cost_estimate=pl.CostEstimate(flops=4 * row_blocks * steps * width**3, bytes_accessed=6 * 10**6, transcendentals=0),
        name="column",
    )(masks, *values, lower)


def corner_kernel(masks, *refs):
    *sum_refs, u_ref, v_ref, dinv_ref, _, out_ref, x_ref, h_ref, sem_ref = refs
    steps, width, _ = dinv_ref.shape
    p, q, _, _ = place_of(masks)
    for n, ref in enumerate(sum_refs):
        slot = (q + steps - n % 3 * 2) % steps
        h_ref[slot if n < 3 else slot + 1 - slot % 2 * 2] = ref[...]
    for k in reversed(range(steps)):
        here = pl.ds(k * width, width)
        later = steps - 1 - k
        if later:
            right = []
            for j in range(k + 1, steps):
                block = stacked(q % 2, u_ref[j, k], v_ref[j, k])
                right.append(jnp.where(masks[CORNER + j, k] > 0, block, jnp.zeros_like(block)))
            right = jnp.concatenate(right, axis=0)
            both = jnp.concatenate([right, right], axis=0)
            rest = pl.ds((k + 1) * width, later * width)
            known = jnp.concatenate(halves(x_ref[rest, rest]), axis=1)
            value = dot(known, both)
            turned = []
            for i in range(k + 1, steps):
                at = (i - k - 1) * width
                block = -(value[at : at + width] + h_ref[i, :, here])
                block = jnp.where(masks[CORNER + i, k] > 0, block, jnp.zeros_like(block))
                x_ref[pl.ds(i * width, width), here] = block
                turned.append(block.T)
            turned = jnp.concatenate(turned, axis=1)
            x_ref[here, rest] = turned
            tail = dot(jnp.concatenate(halves(turned), axis=1), both)
            x_ref[here, here] = dinv_ref[k].T - h_ref[k, :, here] - tail
        else:
            x_ref[here, here] = dinv_ref[k].T - h_ref[k, :, here]
    for k in range(steps):
        for j in range(steps):

            @pl.when((p == k) & (q == j))
            def _():
                block = x_ref.at[pl.ds(k * width, width), pl.ds(j * width, width)]
                copy = pltpu.make_async_copy(block, out_ref.at[0, 0], sem_ref)
                copy.start()
                copy.wait()


def corner_blocks(masks, sums, corner, dinv, whole):
    steps, width, _ = dinv.shape
    return pl.pallas_call(
        corner_kernel,
        in_specs=[SMEM] + [VMEM] * (len(sums) + 3) + [ANY],
        out_specs=ANY,
        out_shape=jax.ShapeDtypeStruct(whole.shape, F32),
        scratch_shapes=[
            pltpu.VMEM((steps * width, steps * width), F32),
            pltpu.VMEM((steps, width, steps * width), F32),
            pltpu.SemaphoreType.DMA,
        ],
        input_output_aliases={4 + len(sums): 0},
        cost_estimate=pl.CostEstimate(flops=10**9, bytes_accessed=10**6, transcendentals=0),
        name="corner",
    )(masks, *sums, *corner, dinv, whole)


def patch_kernel(masks, *refs):
    *value_refs, _, out_ref, turned_ref, sem_ref = refs
    row_blocks, cols, width, _ = out_ref.shape
    p, q, _, _ = place_of(masks)
    has_row, has_col = p < COLS - CORNER, q < COLS - CORNER
    row_first, col_first = has_row & (q >= COLS - CORNER), has_col & (p >= COLS - CORNER)
    rows, columns = [], []
    for row_ref, even_ref, odd_ref in zip(value_refs[::3], value_refs[1::3], value_refs[2::3]):
        for c in range(row_ref.shape[1] // width):
            rows.append((row_ref, pl.ds(c * width, width)))
            columns.append((even_ref, pl.ds(c * width, width)))
            columns.append((odd_ref, pl.ds(c * width, width)))

    def row_copy(c):
        return pltpu.make_async_copy(rows[c][0].at[:, rows[c][1]], out_ref.at[0, c], sem_ref.at[c])

    def col_copy(a):
        return pltpu.make_async_copy(turned_ref.at[a], out_ref.at[a, 0], sem_ref.at[cols + a])

    @pl.when(has_row)
    def _():
        for c in range(1, cols):
            row_copy(c).start()

    @pl.when(row_first)
    def _():
        row_copy(0).start()

    @pl.when(has_col)
    def _():
        for a in range(row_blocks):
            turned_ref[a] = columns[a][0][:, columns[a][1]].T
        for a in range(1, row_blocks):
            col_copy(a).start()
        for a in range(1, row_blocks):
            col_copy(a).wait()

    @pl.when(col_first)
    def _():
        col_copy(0).start()
        col_copy(0).wait()

    @pl.when(has_row)
    def _():
        for c in range(1, cols):
            row_copy(c).wait()

    @pl.when(row_first)
    def _():
        row_copy(0).wait()


def patch(masks, values, whole):
    row_blocks, cols, width, _ = whole.shape
    return pl.pallas_call(
        patch_kernel,
        in_specs=[SMEM] + [VMEM] * len(values) + [ANY],
        out_specs=ANY,
        out_shape=jax.ShapeDtypeStruct(whole.shape, F32),
        scratch_shapes=[pltpu.VMEM((row_blocks, width, width), F32), pltpu.SemaphoreType.DMA((row_blocks + cols,))],
        input_output_aliases={1 + len(values): 0},
        cost_estimate=pl.CostEstimate(flops=10**8, bytes_accessed=4 * 10**6, transcendentals=0),
        name="patch",
    )(masks, *values, whole)


def per_device(ainv_in, ufactor, dinv, pattern):
    row_blocks, _, cols, _, width, _ = ainv_in.shape
    steps = dinv.shape[0]
    n_row, n_col = lax.axis_size("prow"), lax.axis_size("pcol")
    blocks = ainv_in.reshape(row_blocks, cols, width, width)
    lower = ufactor.reshape(row_blocks, steps, width, width)
    p, q = lax.axis_index("prow"), lax.axis_index("pcol")
    z, y, core = p // 2, p % 2, q % 2
    n_z = n_row // 2
    row_ids = jnp.arange(row_blocks, dtype=jnp.int32) * n_row + p
    col_ids = jnp.arange(cols, dtype=jnp.int32) * n_col + q

    flags = pattern[:, :steps]
    mine = lax.dynamic_index_in_dim(flags.reshape(row_blocks, n_row, steps), p, 1, keepdims=False)
    live = (mine > 0) & (row_ids >= steps)[:, None]
    mine = lax.dynamic_index_in_dim(flags.reshape(cols, n_col, steps), q, 1, keepdims=False)
    live_cols = (mine > 0) & (col_ids >= steps)[:, None]
    ids = jnp.where(jnp.arange(steps) == 0, p, q).astype(jnp.int32)
    masks = jnp.concatenate([live.astype(jnp.int32), flags[:steps], live_cols.astype(jnp.int32), ids[None]])

    def at(zz, yy):
        return zz % n_z * 2 + yy

    flip_y = [(d, d ^ 1) for d in range(n_row)]
    flip_z = [(d, d ^ 2) for d in range(n_row)]
    mirror = [(d, at(n_z - 1 - d // 2, d % 2)) for d in range(n_row)]
    flip_core = [(d, d ^ 1) for d in range(n_col)]

    half = width // 2
    mine = lax.dynamic_slice(lower, (0, 0, core * half, 0), (1, steps, half, width))

    def join(bit, own, other):
        return jnp.where(bit == 0, jnp.concatenate([own, other]), jnp.concatenate([other, own]))

    def ring(shift):
        return [(at(zz, yy), at(zz + shift, yy)) for zz in range(n_z) for yy in range(2)]

    pair = join(y, mine, lax.ppermute(mine, "prow", flip_y))
    moved = [pair] + [lax.ppermute(pair, "prow", ring(shift)) for shift in (1, 2, 3)]
    corner = []
    for t in range(steps // 2):
        away = (z - t) % n_z
        corner.append(jnp.where(away == 0, moved[0], jnp.where(away == 1, moved[1], jnp.where(away == 2, moved[2], moved[3]))))
    corner = jnp.concatenate(corner)
    corner = corner, lax.ppermute(corner, "pcol", flip_core)

    both, grid = ("prow", "pcol"), [(x, h, c) for x in range(n_col // 4) for h in range(2) for c in range(2)]

    def device(x, h, c, zz, yy):
        return at(zz, yy) * n_col + x * 4 + h * 2 + c

    whole, parts = None, []
    for first, count in PARTS:
        whole, part = products(blocks, lower, masks, whole, first, count)
        parts.append(part)

    over_m = [(s, d) for s, d in mirror if d < steps]
    over_y = [(s, d) for s, d in flip_y if d < steps]
    over_z = [(s, d) for s, d in flip_z if d < steps]
    routes = (flip_y, flip_z, over_m), (flip_z, over_m, over_y), (mirror, flip_y, over_z)
    pieces = eliminate(masks, parts, corner)
    held = [(pieces[2 * n], pieces[2 * n + 1]) for n in range(len(SIZES))]
    for stage in range(3):
        held = [(lax.ppermute(send, "prow", routes[n][stage]), keep) for n, (send, keep) in enumerate(held)]
        if stage < 2:
            held = [halving(masks, n, stage + 2, keep, came) for n, (came, keep) in enumerate(held)]
    row = masked_row(masks, [v for came, keep in held for v in (keep, came)])

    def turn(k, x, h, c):
        return at(k // 2, k % 2) * n_col + x * 4 + h * 2 + c, device(x, k // 2 % 2, k % 2, x % 2 * 2 + h, c)

    places = [(h, c, zz, yy) for h in range(2) for c in range(2) for zz in range(n_z) for yy in range(2)]

    def slide(place, start, end):
        h, c, zz, yy = place
        return device(start, h, c, zz, yy), device(end, h, c, zz, yy)

    x = q // 4
    first = lax.ppermute(row, both, [turn(k, *place) for k in range(4) for place in grid])
    second = lax.ppermute(row, both, [turn(k, *place) for k in range(4, steps) for place in grid])
    odd0 = lax.ppermute(first, both, [slide(pl_, pl_[2] // 2 + 2, 0) for pl_ in places])
    odd1 = lax.ppermute(second, both, [slide(pl_, pl_[2] // 2 + 2, 1) for pl_ in places if pl_[0] == 0])
    route = [slide(pl_, 0, 1) for pl_ in places if pl_[2] // 2 == 0 and pl_[0] == 0]
    route += [slide(pl_, 1, 0) for pl_ in places if pl_[2] // 2 == 1]
    moved = lax.ppermute(jnp.where(x == 0, second, first), both, route)
    mine = jnp.where(x == 0, first, second)
    values = [row, jnp.where(x == z // 2, mine, moved), jnp.where(x == 0, odd0, odd1)]

    upper, under = column_products(values[1:], lower, masks)

    def here(perm):
        return [(s * n_col + d, t * n_col + d) for s, t in perm for d in range(steps)]

    orders = (flip_y, flip_z), (flip_z, mirror), (mirror, flip_y)
    for (one, two) in orders:
        came = lax.ppermute(upper, both, here(one)), lax.ppermute(under, both, here(two))
        upper, under = upper + came[0], under + came[1]
    sums = jnp.concatenate([upper, under])

    def around(t):
        route = []
        for d in range(steps):
            to = (d + t) % steps
            flip = d // 2 % 2 ^ to // 2 % 2
            route += [(s * n_col + d, (s ^ flip) * n_col + to) for s in range(n_row)]
        return route

    turns = [lax.ppermute(sums, both, around(t)) for t in (2, 4)]
    sums = [sums, *turns]
    sums += [lax.ppermute(v, "pcol", [(d, d ^ 1) for d in range(steps)]) for v in sums]
    whole = patch(masks, values, whole)
    whole = corner_blocks(masks, sums, corner, dinv, whole)
    return whole.reshape(ainv_in.shape)


def solution(mesh):
    placed = (
        P(None, "prow", None, "pcol", None, None),
        P(None, "prow", None, None, None),
        P(),
        P(),
    )
    return jax.shard_map(
        per_device,
        mesh=mesh,
        in_specs=placed,
        out_specs=P(None, "prow", None, "pcol", None, None),
        check_vma=False,
    )
```

```python
import functools

import jax
import jax.numpy as jnp
from jax import lax
from jax.experimental import pallas as pl
from jax.experimental.pallas import tpu as pltpu
from jax.sharding import PartitionSpec as P


F32, BF16 = jnp.float32, jnp.bfloat16
BATCHES = ((0, 1), (2,))
SIZES = (3, 4, 4)
CORNER, COLS, IDS = 18, 24, 33
VMEM = pl.BlockSpec(memory_space=pltpu.VMEM)
SMEM = pl.BlockSpec(memory_space=pltpu.SMEM)
ANY = pl.BlockSpec(memory_space=pl.ANY)


def halves(value):
    high = value.astype(BF16)
    return high, (value - high.astype(F32)).astype(BF16)


def stacked(core, own, other):
    return jnp.concatenate([jnp.where(core > 0, other, own), jnp.where(core > 0, own, other)], axis=0)


def dot(left, right):
    return jnp.dot(left, right, preferred_element_type=F32)


def turned_kernel(masks, u_ref, out_ref):
    rows, steps, width, _ = u_ref.shape
    first = pl.program_id(0) * rows
    for k in range(steps):
        blocks = []
        for r in range(rows):
            block = u_ref[r, k]
            blocks.append(jnp.where(masks[first + r, k] > 0, block, jnp.zeros_like(block)))
        out_ref[pl.ds(k * width, width), :] = jnp.concatenate(blocks, axis=0).T


def turned_factor(masks, lower, rows=6):
    row_blocks, steps, width, _ = lower.shape
    return pl.pallas_call(
        turned_kernel,
        grid_spec=pltpu.PrefetchScalarGridSpec(
            num_scalar_prefetch=1,
            grid=(row_blocks // rows,),
            in_specs=[pl.BlockSpec((rows, steps, width, width), lambda i, _: (i, 0, 0, 0))],
            out_specs=pl.BlockSpec((steps * width, rows * width), lambda i, _: (0, i)),
        ),
        out_shape=jax.ShapeDtypeStruct((steps * width, row_blocks * width), BF16),
        cost_estimate=pl.CostEstimate(flops=2 * 10**9, bytes_accessed=4 * lower.size, transcendentals=0),
        name="turned",
    )(masks, lower)


def product_kernel(x_ref, u_ref, *refs):
    copy_ref, out_ref = refs[-2:]
    step = pl.program_id(0)
    rows, cols, _, _ = x_ref.shape
    high, low = [], []
    for r in range(rows):
        a, b = halves(jnp.concatenate([x_ref[r, c] for c in range(cols)], axis=1))
        high.append(a)
        low.append(b)
    copy_ref[...] = x_ref[...]
    left = u_ref[...]
    term = dot(left, jnp.concatenate(high, axis=0)) + dot(left, jnp.concatenate(low, axis=0))
    term = term.reshape(out_ref.shape)

    @pl.when(step == 0)
    def _():
        out_ref[...] = term

    @pl.when(step > 0)
    def _():
        out_ref[...] += term


def products(blocks, turned, known, group, rows=6):
    row_blocks, cols, width, _ = blocks.shape
    tall = turned.shape[0]
    cols = cols // len(SIZES)
    return pl.pallas_call(
        product_kernel,
        grid=(row_blocks // rows,),
        in_specs=[
            pl.BlockSpec((rows, cols, width, width), lambda i: (i, group, 0, 0)),
            pl.BlockSpec((tall, rows * width), lambda i: (0, i)),
        ]
        + [ANY] * len(known),
        out_specs=[
            pl.BlockSpec((rows, cols, width, width), lambda i: (i, group, 0, 0)),
            pl.BlockSpec((tall // width, width, cols * width), lambda i: (0, 0, 0)),
        ],
        out_shape=[
            jax.ShapeDtypeStruct(blocks.shape, F32),
            jax.ShapeDtypeStruct((tall // width, width, cols * width), F32),
        ],
        input_output_aliases={2: 0} if known else {},
        cost_estimate=pl.CostEstimate(
            flops=4 * row_blocks * cols * tall * width**2, bytes_accessed=8 * row_blocks * cols * width**2, transcendentals=0
        ),
        name="products",
    )(blocks, turned, *known)


def first_pieces(z, y):
    outer, low, other = (z == 0) | (z == 3), z < 2, 1 - y

    def either(flag, yes, no):
        return [jnp.where(flag, a, b) for a, b in zip(yes, no)]

    ends, middle = (0, 1, 0, 0), (2, 3, 4, 5)
    front, back = (0, 1, 2, 3), (4, 5, 0, 0)
    return [
        [other, 2 + other, 4 + other],
        [y, 2 + y, 4 + y],
        either(outer, middle, ends),
        either(outer, ends, middle),
        either(low, back, front),
        either(low, front, back),
    ]


def later_pieces(group, stage, z, y):
    outer, low, other = (z == 0) | (z == 3), z < 2, 1 - y
    one, two = jnp.where(z == 1, 1, 0), jnp.where(z == 2, 1, 0)
    if stage == 2:
        return [
            ([jnp.where(outer, 1, 0), jnp.where(outer, 2, 0)], [jnp.where(outer, 0, 1), jnp.where(outer, 0, 2)]),
            ([2 * one, 2 * one + 1], [2 * two, 2 * two + 1]),
            ([other, jnp.where(low, 2 + other, other)], [y, jnp.where(low, 2 + y, y)]),
        ][group]
    return [([one], [two]), ([other], [y]), ([jnp.where(z == 0, 1, 0)], [one])][group]


def place_of(masks):
    p, q = masks[IDS, 0], masks[IDS, 1]
    return p, q, p // 2, p % 2


def eliminate_kernel(group, masks, part_ref, u_ref, v_ref, send_ref, keep_ref, w_ref):
    steps = w_ref.shape[0]
    _, q, z, y = place_of(masks)
    high, low = [], []
    for k in reversed(range(steps)):
        total = part_ref[k]
        if high:
            blocks = []
            for j in range(k + 1, steps):
                block = stacked(q % 2, u_ref[j, k], v_ref[j, k])
                blocks.append(jnp.where(masks[CORNER + j, k] > 0, block, jnp.zeros_like(block)).T)
            left = jnp.concatenate(blocks + blocks, axis=1)
            total = total + dot(left, jnp.concatenate(high[::-1] + low[::-1], axis=0))
        total = -total
        w_ref[k] = total
        a, b = halves(total)
        high.append(a)
        low.append(b)
    for ref, pieces in zip((send_ref, keep_ref), first_pieces(z, y)[2 * group : 2 * group + 2]):
        for m, k in enumerate(pieces):
            ref[m] = w_ref[k]


def eliminate(masks, group, part, corner):
    _, width, wide = part.shape
    return pl.pallas_call(
        functools.partial(eliminate_kernel, group),
        in_specs=[SMEM] + [VMEM] * 3,
        out_specs=[VMEM] * 2,
        out_shape=[jax.ShapeDtypeStruct((SIZES[group], width, wide), F32)] * 2,
        scratch_shapes=[pltpu.VMEM(part.shape, F32)],
        cost_estimate=pl.CostEstimate(flops=1000 * part.size, bytes_accessed=20 * part.size, transcendentals=0),
        name="eliminate",
    )(masks, part, *corner)


def halving_kernel(group, stage, masks, stay_ref, came_ref, send_ref, keep_ref):
    _, _, z, y = place_of(masks)
    for ref, pieces in zip((send_ref, keep_ref), later_pieces(group, stage, z, y)):
        for m, n in enumerate(pieces):
            ref[m] = stay_ref[n] + came_ref[n]


def halving(masks, group, stage, stay, came):
    _, width, wide = stay.shape
    return pl.pallas_call(
        functools.partial(halving_kernel, group, stage),
        in_specs=[SMEM, VMEM, VMEM],
        out_specs=[VMEM] * 2,
        out_shape=[jax.ShapeDtypeStruct((4 - stage, width, wide), F32)] * 2,
        cost_estimate=pl.CostEstimate(flops=10**8, bytes_accessed=32 * width * wide, transcendentals=0),
        name="halving",
    )(masks, stay, came)


def row_kernel(first, masks, *refs):
    *given, row_ref = refs
    width = row_ref.shape[0]
    count = given[0].shape[2] // width
    p, _, _, _ = place_of(masks)
    k = jnp.minimum(p, COLS - CORNER - 1)
    for n in range(row_ref.shape[1] // width):
        part = pl.ds(n % count * width, width)
        value = given[n // count * 2][0, :, part] + given[n // count * 2 + 1][0, :, part]
        row_ref[:, pl.ds(n * width, width)] = jnp.where(masks[COLS + first + n, k] > 0, value, jnp.zeros_like(value))


def masked_row(masks, first, given):
    _, width, wide = given[0].shape
    return pl.pallas_call(
        functools.partial(row_kernel, first),
        in_specs=[SMEM] + [VMEM] * len(given),
        out_specs=VMEM,
        out_shape=jax.ShapeDtypeStruct((width, wide * len(given) // 2), F32),
        cost_estimate=pl.CostEstimate(flops=10**7, bytes_accessed=8 * width * wide * len(given), transcendentals=0),
        name="row",
    )(masks, *given)


def column_kernel(first, masks, even_ref, odd_ref, u_ref, *refs):
    *given, upper_ref, lower_ref = refs
    _, steps, width, _ = u_ref.shape
    total = None
    for c in range(even_ref.shape[1] // width):
        part = pl.ds(c * width, width)
        value = jnp.concatenate([even_ref[:, part], odd_ref[:, part]], axis=1)
        left = jnp.concatenate(halves(value), axis=0)
        right = []
        for r in (2 * c, 2 * c + 1):
            wide = []
            for k in range(steps):
                block = u_ref[r, k]
                wide.append(jnp.where(masks[first + r, k] > 0, block, jnp.zeros_like(block)))
            right.append(jnp.concatenate(wide, axis=1))
        term = dot(left, jnp.concatenate(right, axis=0))
        total = term if total is None else total + term
    total = total[:width] + total[width:]
    for n, ref in enumerate((upper_ref, lower_ref)):
        value = total[n * width // 2 : (n + 1) * width // 2]
        ref[...] = value + given[n][...] if given else value


def column_products(masks, first, even, odd, lower, given):
    _, steps, width, _ = lower.shape
    count = 2 * even.shape[1] // width
    place = first // count
    return pl.pallas_call(
        functools.partial(column_kernel, first),
        grid=(1,),
        in_specs=[SMEM, VMEM, VMEM, pl.BlockSpec((count, steps, width, width), lambda i: (place, 0, 0, 0))]
        + [VMEM] * len(given),
        out_specs=[VMEM] * 2,
        out_shape=[jax.ShapeDtypeStruct((width // 2, steps * width), F32)] * 2,
        cost_estimate=pl.CostEstimate(flops=4 * count * steps * width**3, bytes_accessed=4 * 10**6, transcendentals=0),
        name="column",
    )(masks, even, odd, lower, *given)


def corner_kernel(masks, *refs):
    *sum_refs, u_ref, v_ref, dinv_ref, _, out_ref, x_ref, h_ref, sem_ref = refs
    steps, width, _ = dinv_ref.shape
    p, q, _, _ = place_of(masks)
    for n, ref in enumerate(sum_refs):
        slot = (q + steps - n % 3 * 2) % steps
        h_ref[slot if n < 3 else slot + 1 - slot % 2 * 2] = ref[...]
    for k in reversed(range(steps)):
        here = pl.ds(k * width, width)
        later = steps - 1 - k
        if later:
            right = []
            for j in range(k + 1, steps):
                block = stacked(q % 2, u_ref[j, k], v_ref[j, k])
                right.append(jnp.where(masks[CORNER + j, k] > 0, block, jnp.zeros_like(block)))
            right = jnp.concatenate(right, axis=0)
            both = jnp.concatenate([right, right], axis=0)
            rest = pl.ds((k + 1) * width, later * width)
            known = jnp.concatenate(halves(x_ref[rest, rest]), axis=1)
            value = dot(known, both)
            turned = []
            for i in range(k + 1, steps):
                at = (i - k - 1) * width
                block = -(value[at : at + width] + h_ref[i, :, here])
                block = jnp.where(masks[CORNER + i, k] > 0, block, jnp.zeros_like(block))
                x_ref[pl.ds(i * width, width), here] = block
                turned.append(block.T)
            turned = jnp.concatenate(turned, axis=1)
            x_ref[here, rest] = turned
            tail = dot(jnp.concatenate(halves(turned), axis=1), both)
            x_ref[here, here] = dinv_ref[k].T - h_ref[k, :, here] - tail
        else:
            x_ref[here, here] = dinv_ref[k].T - h_ref[k, :, here]
    for k in range(steps):
        for j in range(steps):

            @pl.when((p == k) & (q == j))
            def _():
                block = x_ref.at[pl.ds(k * width, width), pl.ds(j * width, width)]
                copy = pltpu.make_async_copy(block, out_ref.at[0, 0], sem_ref)
                copy.start()
                copy.wait()


def corner_blocks(masks, sums, corner, dinv, whole):
    steps, width, _ = dinv.shape
    return pl.pallas_call(
        corner_kernel,
        in_specs=[SMEM] + [VMEM] * (len(sums) + 3) + [ANY],
        out_specs=ANY,
        out_shape=jax.ShapeDtypeStruct(whole.shape, F32),
        scratch_shapes=[
            pltpu.VMEM((steps * width, steps * width), F32),
            pltpu.VMEM((steps, width, steps * width), F32),
            pltpu.SemaphoreType.DMA,
        ],
        input_output_aliases={4 + len(sums): 0},
        cost_estimate=pl.CostEstimate(flops=10**9, bytes_accessed=10**6, transcendentals=0),
        name="corner",
    )(masks, *sums, *corner, dinv, whole)


def patch_kernel(masks, *refs):
    *value_refs, _, out_ref, turned_ref, sem_ref = refs
    row_blocks, cols, width, _ = out_ref.shape
    p, q, _, _ = place_of(masks)
    has_row, has_col = p < COLS - CORNER, q < COLS - CORNER
    row_first, col_first = has_row & (q >= COLS - CORNER), has_col & (p >= COLS - CORNER)
    rows, columns = [], []
    for row_ref, even_ref, odd_ref in zip(value_refs[::3], value_refs[1::3], value_refs[2::3]):
        for c in range(row_ref.shape[1] // width):
            rows.append((row_ref, pl.ds(c * width, width)))
            columns.append((even_ref, pl.ds(c * width, width)))
            columns.append((odd_ref, pl.ds(c * width, width)))

    def row_copy(c):
        return pltpu.make_async_copy(rows[c][0].at[:, rows[c][1]], out_ref.at[0, c], sem_ref.at[c])

    def col_copy(a):
        return pltpu.make_async_copy(turned_ref.at[a], out_ref.at[a, 0], sem_ref.at[cols + a])

    @pl.when(has_row)
    def _():
        for c in range(1, cols):
            row_copy(c).start()

    @pl.when(row_first)
    def _():
        row_copy(0).start()

    @pl.when(has_col)
    def _():
        for a in range(row_blocks):
            turned_ref[a] = columns[a][0][:, columns[a][1]].T
        for a in range(1, row_blocks):
            col_copy(a).start()
        for a in range(1, row_blocks):
            col_copy(a).wait()

    @pl.when(col_first)
    def _():
        col_copy(0).start()
        col_copy(0).wait()

    @pl.when(has_row)
    def _():
        for c in range(1, cols):
            row_copy(c).wait()

    @pl.when(row_first)
    def _():
        row_copy(0).wait()


def patch(masks, values, whole):
    row_blocks, cols, width, _ = whole.shape
    return pl.pallas_call(
        patch_kernel,
        in_specs=[SMEM] + [VMEM] * len(values) + [ANY],
        out_specs=ANY,
        out_shape=jax.ShapeDtypeStruct(whole.shape, F32),
        scratch_shapes=[pltpu.VMEM((row_blocks, width, width), F32), pltpu.SemaphoreType.DMA((row_blocks + cols,))],
        input_output_aliases={1 + len(values): 0},
        cost_estimate=pl.CostEstimate(flops=10**8, bytes_accessed=4 * 10**6, transcendentals=0),
        name="patch",
    )(masks, *values, whole)


def per_device(ainv_in, ufactor, dinv, pattern):
    row_blocks, _, cols, _, width, _ = ainv_in.shape
    steps = dinv.shape[0]
    n_row, n_col = lax.axis_size("prow"), lax.axis_size("pcol")
    blocks = ainv_in.reshape(row_blocks, cols, width, width)
    lower = ufactor.reshape(row_blocks, steps, width, width)
    p, q = lax.axis_index("prow"), lax.axis_index("pcol")
    z, y, core = p // 2, p % 2, q % 2
    n_z = n_row // 2
    row_ids = jnp.arange(row_blocks, dtype=jnp.int32) * n_row + p
    col_ids = jnp.arange(cols, dtype=jnp.int32) * n_col + q

    flags = pattern[:, :steps]
    mine = lax.dynamic_index_in_dim(flags.reshape(row_blocks, n_row, steps), p, 1, keepdims=False)
    live = (mine > 0) & (row_ids >= steps)[:, None]
    mine = lax.dynamic_index_in_dim(flags.reshape(cols, n_col, steps), q, 1, keepdims=False)
    live_cols = (mine > 0) & (col_ids >= steps)[:, None]
    ids = jnp.where(jnp.arange(steps) == 0, p, q).astype(jnp.int32)
    masks = jnp.concatenate([live.astype(jnp.int32), flags[:steps], live_cols.astype(jnp.int32), ids[None]])

    def at(zz, yy):
        return zz % n_z * 2 + yy

    flip_y = [(d, d ^ 1) for d in range(n_row)]
    flip_z = [(d, d ^ 2) for d in range(n_row)]
    mirror = [(d, at(n_z - 1 - d // 2, d % 2)) for d in range(n_row)]
    flip_core = [(d, d ^ 1) for d in range(n_col)]

    half = width // 2
    mine = lax.dynamic_slice(lower, (0, 0, core * half, 0), (1, steps, half, width))

    def join(bit, own, other):
        return jnp.where(bit == 0, jnp.concatenate([own, other]), jnp.concatenate([other, own]))

    def ring(shift):
        return [(at(zz, yy), at(zz + shift, yy)) for zz in range(n_z) for yy in range(2)]

    pair = join(y, mine, lax.ppermute(mine, "prow", flip_y))
    moved = [pair] + [lax.ppermute(pair, "prow", ring(shift)) for shift in (1, 2, 3)]
    corner = []
    for t in range(steps // 2):
        away = (z - t) % n_z
        corner.append(jnp.where(away == 0, moved[0], jnp.where(away == 1, moved[1], jnp.where(away == 2, moved[2], moved[3]))))
    corner = jnp.concatenate(corner)
    corner = corner, lax.ppermute(corner, "pcol", flip_core)

    both, grid = ("prow", "pcol"), [(x, h, c) for x in range(n_col // 4) for h in range(2) for c in range(2)]

    def device(x, h, c, zz, yy):
        return at(zz, yy) * n_col + x * 4 + h * 2 + c

    over_m = [(s, d) for s, d in mirror if d < steps]
    over_y = [(s, d) for s, d in flip_y if d < steps]
    over_z = [(s, d) for s, d in flip_z if d < steps]
    routes = (flip_y, flip_z, over_m), (flip_z, over_m, over_y), (mirror, flip_y, over_z)
    turned = turned_factor(masks, lower)
    known, sums_of = [], []
    for group in range(len(SIZES)):
        whole, part = products(blocks, turned, known, group)
        send, keep = eliminate(masks, group, part, corner)
        known = [whole, keep]
        for stage in range(3):
            came = lax.ppermute(send, "prow", routes[group][stage])
            if stage < 2:
                send, keep = halving(masks, group, stage + 2, keep, came)
        sums_of.append((keep, came))

    def turn(k, x, h, c):
        return at(k // 2, k % 2) * n_col + x * 4 + h * 2 + c, device(x, k // 2 % 2, k % 2, x % 2 * 2 + h, c)

    places = [(h, c, zz, yy) for h in range(2) for c in range(2) for zz in range(n_z) for yy in range(2)]

    def slide(place, start, end):
        h, c, zz, yy = place
        return device(start, h, c, zz, yy), device(end, h, c, zz, yy)

    x = q // 4
    values, upper = [], ()
    for batch in BATCHES:
        start = batch[0] * cols // len(SIZES)
        row = masked_row(masks, start, [v for group in batch for v in sums_of[group]])
        first = lax.ppermute(row, both, [turn(k, *place) for k in range(4) for place in grid])
        second = lax.ppermute(row, both, [turn(k, *place) for k in range(4, steps) for place in grid])
        odd0 = lax.ppermute(first, both, [slide(pl_, pl_[2] // 2 + 2, 0) for pl_ in places])
        odd1 = lax.ppermute(second, both, [slide(pl_, pl_[2] // 2 + 2, 1) for pl_ in places if pl_[0] == 0])
        route = [slide(pl_, 0, 1) for pl_ in places if pl_[2] // 2 == 0 and pl_[0] == 0]
        route += [slide(pl_, 1, 0) for pl_ in places if pl_[2] // 2 == 1]
        moved = lax.ppermute(jnp.where(x == 0, second, first), both, route)
        mine = jnp.where(x == 0, first, second)
        even, odd = jnp.where(x == z // 2, mine, moved), jnp.where(x == 0, odd0, odd1)
        values += [row, even, odd]
        upper = column_products(masks, 2 * start, even, odd, lower, upper)
    upper, under = upper

    def here(perm):
        return [(s * n_col + d, t * n_col + d) for s, t in perm for d in range(steps)]

    orders = (flip_y, flip_z), (flip_z, mirror), (mirror, flip_y)
    for (one, two) in orders:
        came = lax.ppermute(upper, both, here(one)), lax.ppermute(under, both, here(two))
        upper, under = upper + came[0], under + came[1]
    sums = jnp.concatenate([upper, under])

    def around(t):
        route = []
        for d in range(steps):
            to = (d + t) % steps
            flip = d // 2 % 2 ^ to // 2 % 2
            route += [(s * n_col + d, (s ^ flip) * n_col + to) for s in range(n_row)]
        return route

    turns = [lax.ppermute(sums, both, around(t)) for t in (2, 4)]
    sums = [sums, *turns]
    sums += [lax.ppermute(v, "pcol", [(d, d ^ 1) for d in range(steps)]) for v in sums]
    whole = patch(masks, values, whole)
    whole = corner_blocks(masks, sums, corner, dinv, whole)
    return whole.reshape(ainv_in.shape)


def solution(mesh):
    placed = (
        P(None, "prow", None, "pcol", None, None),
        P(None, "prow", None, None, None),
        P(),
        P(),
    )
    return jax.shard_map(
        per_device,
        mesh=mesh,
        in_specs=placed,
        out_specs=P(None, "prow", None, "pcol", None, None),
        check_vma=False,
    )
```

```python
import functools

import jax
import jax.numpy as jnp
from jax import lax
from jax.experimental import pallas as pl
from jax.experimental.pallas import tpu as pltpu
from jax.sharding import PartitionSpec as P


F32, BF16 = jnp.float32, jnp.bfloat16
PARTS = ((0, 18),)
SIZES = (3, 4, 4)
CORNER, COLS, IDS = 18, 24, 33
VMEM = pl.BlockSpec(memory_space=pltpu.VMEM)
SMEM = pl.BlockSpec(memory_space=pltpu.SMEM)
ANY = pl.BlockSpec(memory_space=pl.ANY)


def halves(value):
    high = value.astype(BF16)
    return high, (value - high.astype(F32)).astype(BF16)


def stacked(core, own, other):
    return jnp.concatenate([jnp.where(core > 0, other, own), jnp.where(core > 0, own, other)], axis=0)


def dot(left, right):
    return jnp.dot(left, right, preferred_element_type=F32)


def product_kernel(start, masks, x_ref, u_ref, *refs):
    copy_ref, out_ref = refs[-2:]
    step = pl.program_id(0)
    rows, cols, _, _ = x_ref.shape
    steps = u_ref.shape[1]
    left, high, low = [], [], []
    for r in range(rows):
        wide = []
        for k in range(steps):
            block = u_ref[r, k]
            wide.append(jnp.where(masks[start + step * rows + r, k] > 0, block, jnp.zeros_like(block)))
        left.append(jnp.concatenate(wide, axis=1))
        value = jnp.concatenate([x_ref[r, c] for c in range(cols)], axis=1)
        for c in range(cols):
            copy_ref[r, c] = x_ref[r, c]
        a, b = halves(value)
        high.append(a)
        low.append(b)
    left = jnp.concatenate(left, axis=0).T
    both = jnp.concatenate([left, left], axis=1)
    term = dot(both, jnp.concatenate(high + low, axis=0))
    term = term.reshape(out_ref.shape)

    @pl.when(step == 0)
    def _():
        out_ref[...] = term

    @pl.when(step > 0)
    def _():
        out_ref[...] += term


def products(blocks, lower, masks, whole, first, count, rows=3):
    _, cols, width, _ = blocks.shape
    steps = lower.shape[1]
    start = first // rows
    known = [] if whole is None else [whole]
    return pl.pallas_call(
        functools.partial(product_kernel, first),
        grid_spec=pltpu.PrefetchScalarGridSpec(
            num_scalar_prefetch=1,
            grid=(count // rows,),
            in_specs=[
                pl.BlockSpec((rows, cols, width, width), lambda i, _: (start + i, 0, 0, 0)),
                pl.BlockSpec((rows, steps, width, width), lambda i, _: (start + i, 0, 0, 0)),
            ]
            + [ANY] * len(known),
            out_specs=[
                pl.BlockSpec((rows, cols, width, width), lambda i, _: (start + i, 0, 0, 0)),
                pl.BlockSpec((steps, width, cols * width), lambda i, _: (0, 0, 0)),
            ],
        ),
        out_shape=[
            jax.ShapeDtypeStruct(blocks.shape, F32),
            jax.ShapeDtypeStruct((steps, width, cols * width), F32),
        ],
        input_output_aliases={3: 0} if known else {},
        cost_estimate=pl.CostEstimate(
            flops=4 * count * cols * steps * width**3, bytes_accessed=8 * count * cols * width**2, transcendentals=0
        ),
        name="products",
    )(masks, blocks, lower, *known)


def first_pieces(z, y):
    outer, low, other = (z == 0) | (z == 3), z < 2, 1 - y

    def either(flag, yes, no):
        return [jnp.where(flag, a, b) for a, b in zip(yes, no)]

    ends, middle = (0, 1, 0, 0), (2, 3, 4, 5)
    front, back = (0, 1, 2, 3), (4, 5, 0, 0)
    return [
        [other, 2 + other, 4 + other],
        [y, 2 + y, 4 + y],
        either(outer, middle, ends),
        either(outer, ends, middle),
        either(low, back, front),
        either(low, front, back),
    ]


def later_pieces(group, stage, z, y):
    outer, low, other = (z == 0) | (z == 3), z < 2, 1 - y
    one, two = jnp.where(z == 1, 1, 0), jnp.where(z == 2, 1, 0)
    if stage == 2:
        return [
            ([jnp.where(outer, 1, 0), jnp.where(outer, 2, 0)], [jnp.where(outer, 0, 1), jnp.where(outer, 0, 2)]),
            ([2 * one, 2 * one + 1], [2 * two, 2 * two + 1]),
            ([other, jnp.where(low, 2 + other, other)], [y, jnp.where(low, 2 + y, y)]),
        ][group]
    return [([one], [two]), ([other], [y]), ([jnp.where(z == 0, 1, 0)], [one])][group]


def place_of(masks):
    p, q = masks[IDS, 0], masks[IDS, 1]
    return p, q, p // 2, p % 2


def eliminate_kernel(masks, *refs):
    *part_refs, u_ref, v_ref = refs[: -2 * len(SIZES) - 1]
    places, w_ref = refs[-2 * len(SIZES) - 1 : -1], refs[-1]
    steps = w_ref.shape[0]
    _, q, z, y = place_of(masks)
    high, low = [], []
    for k in reversed(range(steps)):
        total = part_refs[0][k]
        for ref in part_refs[1:]:
            total = total + ref[k]
        if high:
            blocks = []
            for j in range(k + 1, steps):
                block = stacked(q % 2, u_ref[j, k], v_ref[j, k])
                blocks.append(jnp.where(masks[CORNER + j, k] > 0, block, jnp.zeros_like(block)).T)
            left = jnp.concatenate(blocks + blocks, axis=1)
            total = total + dot(left, jnp.concatenate(high[::-1] + low[::-1], axis=0))
        total = -total
        w_ref[k] = total
        a, b = halves(total)
        high.append(a)
        low.append(b)
    for n, (ref, pieces) in enumerate(zip(places, first_pieces(z, y))):
        for m, k in enumerate(pieces):
            ref[m] = w_ref[k, :, pl.ds(n // 2 * ref.shape[2], ref.shape[2])]


def eliminate(masks, parts, corner):
    _, width, wide = parts[0].shape
    shapes = [jax.ShapeDtypeStruct((n, width, wide // len(SIZES)), F32) for n in SIZES for _ in range(2)]
    return pl.pallas_call(
        eliminate_kernel,
        in_specs=[SMEM] + [VMEM] * (len(parts) + 2),
        out_specs=[VMEM] * len(shapes),
        out_shape=shapes,
        scratch_shapes=[pltpu.VMEM(parts[0].shape, F32)],
        cost_estimate=pl.CostEstimate(flops=1000 * parts[0].size, bytes_accessed=20 * parts[0].size, transcendentals=0),
        name="eliminate",
    )(masks, *parts, *corner)


def halving_kernel(masks, stay_a, came_a, stay_b, came_b, send_ref, keep_ref):
    send_ref[...] = stay_a[...] + came_a[...]
    keep_ref[...] = stay_b[...] + came_b[...]


def halving(masks, group, stage, stay, came):
    _, width, wide = stay.shape
    count = 4 - stage

    def piece(side):
        def index(m, masks):
            _, _, z, y = place_of(masks)
            slots = later_pieces(group, stage, z, y)[side]
            slot = slots[0]
            for n in range(1, count):
                slot = jnp.where(m == n, slots[n], slot)
            return slot, 0, 0

        return pl.BlockSpec((1, width, wide), index)

    return pl.pallas_call(
        halving_kernel,
        grid_spec=pltpu.PrefetchScalarGridSpec(
            num_scalar_prefetch=1,
            grid=(count,),
            in_specs=[piece(0), piece(0), piece(1), piece(1)],
            out_specs=[pl.BlockSpec((1, width, wide), lambda m, _: (m, 0, 0))] * 2,
        ),
        out_shape=[jax.ShapeDtypeStruct((count, width, wide), F32)] * 2,
        cost_estimate=pl.CostEstimate(flops=10**8, bytes_accessed=32 * width * wide, transcendentals=0),
        name="halving",
    )(masks, stay, came, stay, came)


def row_kernel(masks, *refs):
    *given, row_ref = refs
    width = row_ref.shape[0]
    count = given[0].shape[2] // width
    p, _, _, _ = place_of(masks)
    k = jnp.minimum(p, COLS - CORNER - 1)
    for n in range(row_ref.shape[1] // width):
        part = pl.ds(n % count * width, width)
        value = given[n // count * 2][0, :, part] + given[n // count * 2 + 1][0, :, part]
        row_ref[:, pl.ds(n * width, width)] = jnp.where(masks[COLS + n, k] > 0, value, jnp.zeros_like(value))


def masked_row(masks, given):
    _, width, wide = given[0].shape
    return pl.pallas_call(
        row_kernel,
        in_specs=[SMEM] + [VMEM] * len(given),
        out_specs=VMEM,
        out_shape=jax.ShapeDtypeStruct((width, wide * len(given) // 2), F32),
        cost_estimate=pl.CostEstimate(flops=10**7, bytes_accessed=8 * width * wide * len(given), transcendentals=0),
        name="row",
    )(masks, *given)


def column_kernel(parity, masks, value_ref, u_ref, *refs):
    *given, upper_ref, lower_ref = refs
    count, _, steps, width, _ = u_ref.shape
    total = None
    for c in range(0, count, 2):
        taken = range(c, min(c + 2, count))
        left = jnp.concatenate(halves(value_ref[:, pl.ds(c * width, len(taken) * width)]), axis=0)
        right = []
        for r in taken:
            wide = []
            for k in range(steps):
                block = u_ref[r, 0, k]
                wide.append(jnp.where(masks[2 * r + parity, k] > 0, block, jnp.zeros_like(block)))
            right.append(jnp.concatenate(wide, axis=1))
        term = dot(left, jnp.concatenate(right, axis=0))
        total = term if total is None else total + term
    total = total[:width] + total[width:]
    for n, ref in enumerate((upper_ref, lower_ref)):
        value = total[n * width // 2 : (n + 1) * width // 2]
        ref[...] = value + given[n][...] if given else value


def column_products(masks, parity, value, lower, given):
    row_blocks, steps, width, _ = lower.shape
    count = row_blocks // 2
    return pl.pallas_call(
        functools.partial(column_kernel, parity),
        grid=(1,),
        in_specs=[SMEM, VMEM, pl.BlockSpec((count, 1, steps, width, width), lambda i: (0, parity, 0, 0, 0))]
        + [VMEM] * len(given),
        out_specs=[VMEM] * 2,
        out_shape=[jax.ShapeDtypeStruct((width // 2, steps * width), F32)] * 2,
        cost_estimate=pl.CostEstimate(flops=4 * count * steps * width**3, bytes_accessed=4 * 10**6, transcendentals=0),
        name="column",
    )(masks, value, lower.reshape(count, 2, steps, width, width), *given)


def corner_kernel(masks, *refs):
    *sum_refs, u_ref, v_ref, dinv_ref, _, out_ref, x_ref, h_ref, sem_ref = refs
    steps, width, _ = dinv_ref.shape
    p, q, _, _ = place_of(masks)
    for n, ref in enumerate(sum_refs):
        slot = (q + steps - n % 3 * 2) % steps
        h_ref[slot if n < 3 else slot + 1 - slot % 2 * 2] = ref[...]
    for k in reversed(range(steps)):
        here = pl.ds(k * width, width)
        later = steps - 1 - k
        if later:
            right = []
            for j in range(k + 1, steps):
                block = stacked(q % 2, u_ref[j, k], v_ref[j, k])
                right.append(jnp.where(masks[CORNER + j, k] > 0, block, jnp.zeros_like(block)))
            right = jnp.concatenate(right, axis=0)
            both = jnp.concatenate([right, right], axis=0)
            rest = pl.ds((k + 1) * width, later * width)
            known = jnp.concatenate(halves(x_ref[rest, rest]), axis=1)
            value = dot(known, both)
            turned = []
            for i in range(k + 1, steps):
                at = (i - k - 1) * width
                block = -(value[at : at + width] + h_ref[i, :, here])
                block = jnp.where(masks[CORNER + i, k] > 0, block, jnp.zeros_like(block))
                x_ref[pl.ds(i * width, width), here] = block
                turned.append(block.T)
            turned = jnp.concatenate(turned, axis=1)
            x_ref[here, rest] = turned
            tail = dot(jnp.concatenate(halves(turned), axis=1), both)
            x_ref[here, here] = dinv_ref[k].T - h_ref[k, :, here] - tail
        else:
            x_ref[here, here] = dinv_ref[k].T - h_ref[k, :, here]
    for k in range(steps):
        for j in range(steps):

            @pl.when((p == k) & (q == j))
            def _():
                block = x_ref.at[pl.ds(k * width, width), pl.ds(j * width, width)]
                copy = pltpu.make_async_copy(block, out_ref.at[0, 0], sem_ref)
                copy.start()
                copy.wait()


def corner_blocks(masks, sums, corner, dinv, whole):
    steps, width, _ = dinv.shape
    return pl.pallas_call(
        corner_kernel,
        in_specs=[SMEM] + [VMEM] * (len(sums) + 3) + [ANY],
        out_specs=ANY,
        out_shape=jax.ShapeDtypeStruct(whole.shape, F32),
        scratch_shapes=[
            pltpu.VMEM((steps * width, steps * width), F32),
            pltpu.VMEM((steps, width, steps * width), F32),
            pltpu.SemaphoreType.DMA,
        ],
        input_output_aliases={4 + len(sums): 0},
        cost_estimate=pl.CostEstimate(flops=10**9, bytes_accessed=10**6, transcendentals=0),
        name="corner",
    )(masks, *sums, *corner, dinv, whole)


def patch_kernel(masks, *refs):
    *value_refs, _, out_ref, turned_ref, sem_ref = refs
    row_blocks, cols, width, _ = out_ref.shape
    p, q, _, _ = place_of(masks)
    has_row, has_col = p < COLS - CORNER, q < COLS - CORNER
    row_first, col_first = has_row & (q >= COLS - CORNER), has_col & (p >= COLS - CORNER)
    rows, columns = [], []
    for row_ref, even_ref, odd_ref in zip(value_refs[::3], value_refs[1::3], value_refs[2::3]):
        for c in range(row_ref.shape[1] // width):
            rows.append((row_ref, pl.ds(c * width, width)))
            columns.append((even_ref, pl.ds(c * width, width)))
            columns.append((odd_ref, pl.ds(c * width, width)))

    def row_copy(c):
        return pltpu.make_async_copy(rows[c][0].at[:, rows[c][1]], out_ref.at[0, c], sem_ref.at[c])

    def col_copy(a):
        return pltpu.make_async_copy(turned_ref.at[a], out_ref.at[a, 0], sem_ref.at[cols + a])

    @pl.when(has_row)
    def _():
        for c in range(1, cols):
            row_copy(c).start()

    @pl.when(row_first)
    def _():
        row_copy(0).start()

    @pl.when(has_col)
    def _():
        for a in range(row_blocks):
            turned_ref[a] = columns[a][0][:, columns[a][1]].T
        for a in range(1, row_blocks):
            col_copy(a).start()
        for a in range(1, row_blocks):
            col_copy(a).wait()

    @pl.when(col_first)
    def _():
        col_copy(0).start()
        col_copy(0).wait()

    @pl.when(has_row)
    def _():
        for c in range(1, cols):
            row_copy(c).wait()

    @pl.when(row_first)
    def _():
        row_copy(0).wait()


def patch(masks, values, whole):
    row_blocks, cols, width, _ = whole.shape
    return pl.pallas_call(
        patch_kernel,
        in_specs=[SMEM] + [VMEM] * len(values) + [ANY],
        out_specs=ANY,
        out_shape=jax.ShapeDtypeStruct(whole.shape, F32),
        scratch_shapes=[pltpu.VMEM((row_blocks, width, width), F32), pltpu.SemaphoreType.DMA((row_blocks + cols,))],
        input_output_aliases={1 + len(values): 0},
        cost_estimate=pl.CostEstimate(flops=10**8, bytes_accessed=4 * 10**6, transcendentals=0),
        name="patch",
    )(masks, *values, whole)


def per_device(ainv_in, ufactor, dinv, pattern):
    row_blocks, _, cols, _, width, _ = ainv_in.shape
    steps = dinv.shape[0]
    n_row, n_col = lax.axis_size("prow"), lax.axis_size("pcol")
    blocks = ainv_in.reshape(row_blocks, cols, width, width)
    lower = ufactor.reshape(row_blocks, steps, width, width)
    p, q = lax.axis_index("prow"), lax.axis_index("pcol")
    z, y, core = p // 2, p % 2, q % 2
    n_z = n_row // 2
    row_ids = jnp.arange(row_blocks, dtype=jnp.int32) * n_row + p
    col_ids = jnp.arange(cols, dtype=jnp.int32) * n_col + q

    flags = pattern[:, :steps]
    mine = lax.dynamic_index_in_dim(flags.reshape(row_blocks, n_row, steps), p, 1, keepdims=False)
    live = (mine > 0) & (row_ids >= steps)[:, None]
    mine = lax.dynamic_index_in_dim(flags.reshape(cols, n_col, steps), q, 1, keepdims=False)
    live_cols = (mine > 0) & (col_ids >= steps)[:, None]
    ids = jnp.where(jnp.arange(steps) == 0, p, q).astype(jnp.int32)
    masks = jnp.concatenate([live.astype(jnp.int32), flags[:steps], live_cols.astype(jnp.int32), ids[None]])

    def at(zz, yy):
        return zz % n_z * 2 + yy

    flip_y = [(d, d ^ 1) for d in range(n_row)]
    flip_z = [(d, d ^ 2) for d in range(n_row)]
    mirror = [(d, at(n_z - 1 - d // 2, d % 2)) for d in range(n_row)]
    flip_core = [(d, d ^ 1) for d in range(n_col)]

    half = width // 2
    mine = lax.dynamic_slice(lower, (0, 0, core * half, 0), (1, steps, half, width))

    def join(bit, own, other):
        return jnp.where(bit == 0, jnp.concatenate([own, other]), jnp.concatenate([other, own]))

    def ring(shift):
        return [(at(zz, yy), at(zz + shift, yy)) for zz in range(n_z) for yy in range(2)]

    pair = join(y, mine, lax.ppermute(mine, "prow", flip_y))
    moved = [pair] + [lax.ppermute(pair, "prow", ring(shift)) for shift in (1, 2, 3)]
    corner = []
    for t in range(steps // 2):
        away = (z - t) % n_z
        corner.append(jnp.where(away == 0, moved[0], jnp.where(away == 1, moved[1], jnp.where(away == 2, moved[2], moved[3]))))
    corner = jnp.concatenate(corner)
    corner = corner, lax.ppermute(corner, "pcol", flip_core)

    both, grid = ("prow", "pcol"), [(x, h, c) for x in range(n_col // 4) for h in range(2) for c in range(2)]

    def device(x, h, c, zz, yy):
        return at(zz, yy) * n_col + x * 4 + h * 2 + c

    whole, parts = None, []
    for first, count in PARTS:
        whole, part = products(blocks, lower, masks, whole, first, count)
        parts.append(part)

    over_m = [(s, d) for s, d in mirror if d < steps]
    over_y = [(s, d) for s, d in flip_y if d < steps]
    over_z = [(s, d) for s, d in flip_z if d < steps]
    routes = (flip_y, flip_z, over_m), (flip_z, over_m, over_y), (mirror, flip_y, over_z)
    pieces = eliminate(masks, parts, corner)
    held = [(pieces[2 * n], pieces[2 * n + 1]) for n in range(len(SIZES))]
    for stage in range(3):
        held = [(lax.ppermute(send, "prow", routes[n][stage]), keep) for n, (send, keep) in enumerate(held)]
        if stage < 2:
            held = [halving(masks, n, stage + 2, keep, came) for n, (came, keep) in enumerate(held)]
    row = masked_row(masks, [v for came, keep in held for v in (keep, came)])

    def turn(k, x, h, c):
        return at(k // 2, k % 2) * n_col + x * 4 + h * 2 + c, device(x, k // 2 % 2, k % 2, x % 2 * 2 + h, c)

    places = [(h, c, zz, yy) for h in range(2) for c in range(2) for zz in range(n_z) for yy in range(2)]

    def slide(place, start, end):
        h, c, zz, yy = place
        return device(start, h, c, zz, yy), device(end, h, c, zz, yy)

    x = q // 4
    first = lax.ppermute(row, both, [turn(k, *place) for k in range(4) for place in grid])
    second = lax.ppermute(row, both, [turn(k, *place) for k in range(4, steps) for place in grid])
    odd0 = lax.ppermute(first, both, [slide(pl_, pl_[2] // 2 + 2, 0) for pl_ in places])
    odd1 = lax.ppermute(second, both, [slide(pl_, pl_[2] // 2 + 2, 1) for pl_ in places if pl_[0] == 0])
    route = [slide(pl_, 0, 1) for pl_ in places if pl_[2] // 2 == 0 and pl_[0] == 0]
    route += [slide(pl_, 1, 0) for pl_ in places if pl_[2] // 2 == 1]
    moved = lax.ppermute(jnp.where(x == 0, second, first), both, route)
    mine = jnp.where(x == 0, first, second)
    values = [row, jnp.where(x == z // 2, mine, moved), jnp.where(x == 0, odd0, odd1)]

    sums = column_products(masks, 0, values[1], lower, ())
    upper, under = column_products(masks, 1, values[2], lower, sums)

    def here(perm):
        return [(s * n_col + d, t * n_col + d) for s, t in perm for d in range(steps)]

    orders = (flip_y, flip_z), (flip_z, mirror), (mirror, flip_y)
    for (one, two) in orders:
        came = lax.ppermute(upper, both, here(one)), lax.ppermute(under, both, here(two))
        upper, under = upper + came[0], under + came[1]
    sums = jnp.concatenate([upper, under])

    def around(t):
        route = []
        for d in range(steps):
            to = (d + t) % steps
            flip = d // 2 % 2 ^ to // 2 % 2
            route += [(s * n_col + d, (s ^ flip) * n_col + to) for s in range(n_row)]
        return route

    turns = [lax.ppermute(sums, both, around(t)) for t in (2, 4)]
    sums = [sums, *turns]
    sums += [lax.ppermute(v, "pcol", [(d, d ^ 1) for d in range(steps)]) for v in sums]
    whole = patch(masks, values, whole)
    whole = corner_blocks(masks, sums, corner, dinv, whole)
    return whole.reshape(ainv_in.shape)


def solution(mesh):
    placed = (
        P(None, "prow", None, "pcol", None, None),
        P(None, "prow", None, None, None),
        P(),
        P(),
    )
    return jax.shard_map(
        per_device,
        mesh=mesh,
        in_specs=placed,
        out_specs=P(None, "prow", None, "pcol", None, None),
        check_vma=False,
    )
```

```python
import functools

import jax
import jax.numpy as jnp
from jax import lax
from jax.experimental import pallas as pl
from jax.experimental.pallas import tpu as pltpu
from jax.sharding import PartitionSpec as P


F32, BF16 = jnp.float32, jnp.bfloat16
PARTS = ((0, 18),)
SIZES = (3, 4, 4)
CORNER, COLS, IDS = 18, 24, 33
VMEM = pl.BlockSpec(memory_space=pltpu.VMEM)
SMEM = pl.BlockSpec(memory_space=pltpu.SMEM)
ANY = pl.BlockSpec(memory_space=pl.ANY)


def halves(value):
    high = value.astype(BF16)
    return high, (value - high.astype(F32)).astype(BF16)


def stacked(core, own, other):
    return jnp.concatenate([jnp.where(core > 0, other, own), jnp.where(core > 0, own, other)], axis=0)


def dot(left, right):
    return jnp.dot(left, right, preferred_element_type=F32)


def product_kernel(start, masks, x_ref, u_ref, *refs):
    copy_ref, out_ref = refs[-2:]
    step = pl.program_id(0)
    rows, cols, _, _ = x_ref.shape
    steps = u_ref.shape[1]
    left, high, low = [], [], []
    for r in range(rows):
        wide = []
        for k in range(steps):
            block = u_ref[r, k]
            wide.append(jnp.where(masks[start + step * rows + r, k] > 0, block, jnp.zeros_like(block)))
        left.append(jnp.concatenate(wide, axis=1))
        value = jnp.concatenate([x_ref[r, c] for c in range(cols)], axis=1)
        for c in range(cols):
            copy_ref[r, c] = x_ref[r, c]
        a, b = halves(value)
        high.append(a)
        low.append(b)
    left = jnp.concatenate(left, axis=0).T
    both = jnp.concatenate([left, left], axis=1)
    term = dot(both, jnp.concatenate(high + low, axis=0))
    term = term.reshape(out_ref.shape)

    @pl.when(step == 0)
    def _():
        out_ref[...] = term

    @pl.when(step > 0)
    def _():
        out_ref[...] += term


def products(blocks, lower, masks, whole, first, count, rows=3):
    _, cols, width, _ = blocks.shape
    steps = lower.shape[1]
    start = first // rows
    known = [] if whole is None else [whole]
    return pl.pallas_call(
        functools.partial(product_kernel, first),
        grid_spec=pltpu.PrefetchScalarGridSpec(
            num_scalar_prefetch=1,
            grid=(count // rows,),
            in_specs=[
                pl.BlockSpec((rows, cols, width, width), lambda i, _: (start + i, 0, 0, 0)),
                pl.BlockSpec((rows, steps, width, width), lambda i, _: (start + i, 0, 0, 0)),
            ]
            + [ANY] * len(known),
            out_specs=[
                pl.BlockSpec((rows, cols, width, width), lambda i, _: (start + i, 0, 0, 0)),
                pl.BlockSpec((steps, width, cols * width), lambda i, _: (0, 0, 0)),
            ],
        ),
        out_shape=[
            jax.ShapeDtypeStruct(blocks.shape, F32),
            jax.ShapeDtypeStruct((steps, width, cols * width), F32),
        ],
        input_output_aliases={3: 0} if known else {},
        cost_estimate=pl.CostEstimate(
            flops=4 * count * cols * steps * width**3, bytes_accessed=8 * count * cols * width**2, transcendentals=0
        ),
        name="products",
    )(masks, blocks, lower, *known)


def first_pieces(z, y):
    outer, low, other = (z == 0) | (z == 3), z < 2, 1 - y

    def either(flag, yes, no):
        return [jnp.where(flag, a, b) for a, b in zip(yes, no)]

    ends, middle = (0, 1, 0, 0), (2, 3, 4, 5)
    front, back = (0, 1, 2, 3), (4, 5, 0, 0)
    return [
        [other, 2 + other, 4 + other],
        [y, 2 + y, 4 + y],
        either(outer, middle, ends),
        either(outer, ends, middle),
        either(low, back, front),
        either(low, front, back),
    ]


def later_pieces(group, stage, z, y):
    outer, low, other = (z == 0) | (z == 3), z < 2, 1 - y
    one, two = jnp.where(z == 1, 1, 0), jnp.where(z == 2, 1, 0)
    if stage == 2:
        return [
            ([jnp.where(outer, 1, 0), jnp.where(outer, 2, 0)], [jnp.where(outer, 0, 1), jnp.where(outer, 0, 2)]),
            ([2 * one, 2 * one + 1], [2 * two, 2 * two + 1]),
            ([other, jnp.where(low, 2 + other, other)], [y, jnp.where(low, 2 + y, y)]),
        ][group]
    return [([one], [two]), ([other], [y]), ([jnp.where(z == 0, 1, 0)], [one])][group]


def place_of(masks):
    p, q = masks[IDS, 0], masks[IDS, 1]
    return p, q, p // 2, p % 2


def eliminate_kernel(masks, *refs):
    *part_refs, u_ref, v_ref = refs[: -2 * len(SIZES) - 1]
    places, w_ref = refs[-2 * len(SIZES) - 1 : -1], refs[-1]
    steps = w_ref.shape[0]
    _, q, z, y = place_of(masks)
    high, low = [], []
    for k in reversed(range(steps)):
        total = part_refs[0][k]
        for ref in part_refs[1:]:
            total = total + ref[k]
        if high:
            blocks = []
            for j in range(k + 1, steps):
                block = stacked(q % 2, u_ref[j, k], v_ref[j, k])
                blocks.append(jnp.where(masks[CORNER + j, k] > 0, block, jnp.zeros_like(block)).T)
            left = jnp.concatenate(blocks + blocks, axis=1)
            total = total + dot(left, jnp.concatenate(high[::-1] + low[::-1], axis=0))
        total = -total
        w_ref[k] = total
        a, b = halves(total)
        high.append(a)
        low.append(b)
    for n, (ref, pieces) in enumerate(zip(places, first_pieces(z, y))):
        for m, k in enumerate(pieces):
            ref[m] = w_ref[k, :, pl.ds(n // 2 * ref.shape[2], ref.shape[2])]


def eliminate(masks, parts, corner):
    _, width, wide = parts[0].shape
    shapes = [jax.ShapeDtypeStruct((n, width, wide // len(SIZES)), F32) for n in SIZES for _ in range(2)]
    return pl.pallas_call(
        eliminate_kernel,
        in_specs=[SMEM] + [VMEM] * (len(parts) + 2),
        out_specs=[VMEM] * len(shapes),
        out_shape=shapes,
        scratch_shapes=[pltpu.VMEM(parts[0].shape, F32)],
        cost_estimate=pl.CostEstimate(flops=1000 * parts[0].size, bytes_accessed=20 * parts[0].size, transcendentals=0),
        compiler_params=pltpu.CompilerParams(vmem_limit_bytes=24 * 2**20),
        name="eliminate",
    )(masks, *parts, *corner)


def halving_kernel(group, stage, masks, stay_ref, came_ref, send_ref, keep_ref):
    _, _, z, y = place_of(masks)
    for ref, pieces in zip((send_ref, keep_ref), later_pieces(group, stage, z, y)):
        for m, n in enumerate(pieces):
            ref[m] = stay_ref[n] + came_ref[n]


def halving(masks, group, stage, stay, came):
    _, width, wide = stay.shape
    return pl.pallas_call(
        functools.partial(halving_kernel, group, stage),
        in_specs=[SMEM, VMEM, VMEM],
        out_specs=[VMEM] * 2,
        out_shape=[jax.ShapeDtypeStruct((4 - stage, width, wide), F32)] * 2,
        cost_estimate=pl.CostEstimate(flops=10**8, bytes_accessed=32 * width * wide, transcendentals=0),
        compiler_params=pltpu.CompilerParams(vmem_limit_bytes=8 * 2**20),
        name="halving",
    )(masks, stay, came)


def row_kernel(masks, *refs):
    *given, row_ref = refs
    width = row_ref.shape[0]
    count = given[0].shape[2] // width
    p, _, _, _ = place_of(masks)
    k = jnp.minimum(p, COLS - CORNER - 1)
    for n in range(row_ref.shape[1] // width):
        part = pl.ds(n % count * width, width)
        value = given[n // count * 2][0, :, part] + given[n // count * 2 + 1][0, :, part]
        row_ref[:, pl.ds(n * width, width)] = jnp.where(masks[COLS + n, k] > 0, value, jnp.zeros_like(value))


def masked_row(masks, given):
    _, width, wide = given[0].shape
    return pl.pallas_call(
        row_kernel,
        in_specs=[SMEM] + [VMEM] * len(given),
        out_specs=VMEM,
        out_shape=jax.ShapeDtypeStruct((width, wide * len(given) // 2), F32),
        cost_estimate=pl.CostEstimate(flops=10**7, bytes_accessed=8 * width * wide * len(given), transcendentals=0),
        compiler_params=pltpu.CompilerParams(vmem_limit_bytes=12 * 2**20),
        name="row",
    )(masks, *given)


def column_kernel(parity, masks, value_ref, u_ref, *refs):
    *given, upper_ref, lower_ref = refs
    count, _, steps, width, _ = u_ref.shape
    total = None
    for c in range(0, count, 2):
        taken = range(c, min(c + 2, count))
        left = jnp.concatenate(halves(value_ref[:, pl.ds(c * width, len(taken) * width)]), axis=0)
        right = []
        for r in taken:
            wide = []
            for k in range(steps):
                block = u_ref[r, 0, k]
                wide.append(jnp.where(masks[2 * r + parity, k] > 0, block, jnp.zeros_like(block)))
            right.append(jnp.concatenate(wide, axis=1))
        term = dot(left, jnp.concatenate(right, axis=0))
        total = term if total is None else total + term
    total = total[:width] + total[width:]
    for n, ref in enumerate((upper_ref, lower_ref)):
        value = total[n * width // 2 : (n + 1) * width // 2]
        ref[...] = value + given[n][...] if given else value


def column_products(masks, parity, value, lower, given):
    row_blocks, steps, width, _ = lower.shape
    count = row_blocks // 2
    return pl.pallas_call(
        functools.partial(column_kernel, parity),
        grid=(1,),
        in_specs=[SMEM, VMEM, pl.BlockSpec((count, 1, steps, width, width), lambda i: (0, parity, 0, 0, 0))]
        + [VMEM] * len(given),
        out_specs=[VMEM] * 2,
        out_shape=[jax.ShapeDtypeStruct((width // 2, steps * width), F32)] * 2,
        cost_estimate=pl.CostEstimate(flops=4 * count * steps * width**3, bytes_accessed=4 * 10**6, transcendentals=0),
        compiler_params=pltpu.CompilerParams(vmem_limit_bytes=16 * 2**20),
        name="column",
    )(masks, value, lower.reshape(count, 2, steps, width, width), *given)


def corner_kernel(masks, *refs):
    *sum_refs, u_ref, v_ref, dinv_ref, _, out_ref, x_ref, h_ref, sem_ref = refs
    steps, width, _ = dinv_ref.shape
    p, q, _, _ = place_of(masks)
    for n, ref in enumerate(sum_refs):
        slot = (q + steps - n % 3 * 2) % steps
        h_ref[slot if n < 3 else slot + 1 - slot % 2 * 2] = ref[...]
    for k in reversed(range(steps)):
        here = pl.ds(k * width, width)
        later = steps - 1 - k
        if later:
            right = []
            for j in range(k + 1, steps):
                block = stacked(q % 2, u_ref[j, k], v_ref[j, k])
                right.append(jnp.where(masks[CORNER + j, k] > 0, block, jnp.zeros_like(block)))
            right = jnp.concatenate(right, axis=0)
            both = jnp.concatenate([right, right], axis=0)
            rest = pl.ds((k + 1) * width, later * width)
            known = jnp.concatenate(halves(x_ref[rest, rest]), axis=1)
            value = dot(known, both)
            turned = []
            for i in range(k + 1, steps):
                at = (i - k - 1) * width
                block = -(value[at : at + width] + h_ref[i, :, here])
                block = jnp.where(masks[CORNER + i, k] > 0, block, jnp.zeros_like(block))
                x_ref[pl.ds(i * width, width), here] = block
                turned.append(block.T)
            turned = jnp.concatenate(turned, axis=1)
            x_ref[here, rest] = turned
            tail = dot(jnp.concatenate(halves(turned), axis=1), both)
            x_ref[here, here] = dinv_ref[k].T - h_ref[k, :, here] - tail
        else:
            x_ref[here, here] = dinv_ref[k].T - h_ref[k, :, here]
    for k in range(steps):
        for j in range(steps):

            @pl.when((p == k) & (q == j))
            def _():
                block = x_ref.at[pl.ds(k * width, width), pl.ds(j * width, width)]
                copy = pltpu.make_async_copy(block, out_ref.at[0, 0], sem_ref)
                copy.start()
                copy.wait()


def corner_blocks(masks, sums, corner, dinv, whole):
    steps, width, _ = dinv.shape
    return pl.pallas_call(
        corner_kernel,
        in_specs=[SMEM] + [VMEM] * (len(sums) + 3) + [ANY],
        out_specs=ANY,
        out_shape=jax.ShapeDtypeStruct(whole.shape, F32),
        scratch_shapes=[
            pltpu.VMEM((steps * width, steps * width), F32),
            pltpu.VMEM((steps, width, steps * width), F32),
            pltpu.SemaphoreType.DMA,
        ],
        input_output_aliases={4 + len(sums): 0},
        cost_estimate=pl.CostEstimate(flops=10**9, bytes_accessed=10**6, transcendentals=0),
        name="corner",
    )(masks, *sums, *corner, dinv, whole)


def patch_kernel(masks, *refs):
    *value_refs, _, out_ref, turned_ref, sem_ref = refs
    row_blocks, cols, width, _ = out_ref.shape
    p, q, _, _ = place_of(masks)
    has_row, has_col = p < COLS - CORNER, q < COLS - CORNER
    row_first, col_first = has_row & (q >= COLS - CORNER), has_col & (p >= COLS - CORNER)
    rows, columns = [], []
    for row_ref, even_ref, odd_ref in zip(value_refs[::3], value_refs[1::3], value_refs[2::3]):
        for c in range(row_ref.shape[1] // width):
            rows.append((row_ref, pl.ds(c * width, width)))
            columns.append((even_ref, pl.ds(c * width, width)))
            columns.append((odd_ref, pl.ds(c * width, width)))

    def row_copy(c):
        return pltpu.make_async_copy(rows[c][0].at[:, rows[c][1]], out_ref.at[0, c], sem_ref.at[c])

    def col_copy(a):
        return pltpu.make_async_copy(turned_ref.at[a], out_ref.at[a, 0], sem_ref.at[cols + a])

    @pl.when(has_row)
    def _():
        for c in range(1, cols):
            row_copy(c).start()

    @pl.when(row_first)
    def _():
        row_copy(0).start()

    @pl.when(has_col)
    def _():
        for a in range(row_blocks):
            turned_ref[a] = columns[a][0][:, columns[a][1]].T
        for a in range(1, row_blocks):
            col_copy(a).start()
        for a in range(1, row_blocks):
            col_copy(a).wait()

    @pl.when(col_first)
    def _():
        col_copy(0).start()
        col_copy(0).wait()

    @pl.when(has_row)
    def _():
        for c in range(1, cols):
            row_copy(c).wait()

    @pl.when(row_first)
    def _():
        row_copy(0).wait()


def patch(masks, values, whole):
    row_blocks, cols, width, _ = whole.shape
    return pl.pallas_call(
        patch_kernel,
        in_specs=[SMEM] + [VMEM] * len(values) + [ANY],
        out_specs=ANY,
        out_shape=jax.ShapeDtypeStruct(whole.shape, F32),
        scratch_shapes=[pltpu.VMEM((row_blocks, width, width), F32), pltpu.SemaphoreType.DMA((row_blocks + cols,))],
        input_output_aliases={1 + len(values): 0},
        cost_estimate=pl.CostEstimate(flops=10**8, bytes_accessed=4 * 10**6, transcendentals=0),
        name="patch",
    )(masks, *values, whole)


def per_device(ainv_in, ufactor, dinv, pattern):
    row_blocks, _, cols, _, width, _ = ainv_in.shape
    steps = dinv.shape[0]
    n_row, n_col = lax.axis_size("prow"), lax.axis_size("pcol")
    blocks = ainv_in.reshape(row_blocks, cols, width, width)
    lower = ufactor.reshape(row_blocks, steps, width, width)
    p, q = lax.axis_index("prow"), lax.axis_index("pcol")
    z, y, core = p // 2, p % 2, q % 2
    n_z = n_row // 2
    row_ids = jnp.arange(row_blocks, dtype=jnp.int32) * n_row + p
    col_ids = jnp.arange(cols, dtype=jnp.int32) * n_col + q

    flags = pattern[:, :steps]
    mine = lax.dynamic_index_in_dim(flags.reshape(row_blocks, n_row, steps), p, 1, keepdims=False)
    live = (mine > 0) & (row_ids >= steps)[:, None]
    mine = lax.dynamic_index_in_dim(flags.reshape(cols, n_col, steps), q, 1, keepdims=False)
    live_cols = (mine > 0) & (col_ids >= steps)[:, None]
    ids = jnp.where(jnp.arange(steps) == 0, p, q).astype(jnp.int32)
    masks = jnp.concatenate([live.astype(jnp.int32), flags[:steps], live_cols.astype(jnp.int32), ids[None]])

    def at(zz, yy):
        return zz % n_z * 2 + yy

    flip_y = [(d, d ^ 1) for d in range(n_row)]
    flip_z = [(d, d ^ 2) for d in range(n_row)]
    mirror = [(d, at(n_z - 1 - d // 2, d % 2)) for d in range(n_row)]
    flip_core = [(d, d ^ 1) for d in range(n_col)]

    half = width // 2
    mine = lax.dynamic_slice(lower, (0, 0, core * half, 0), (1, steps, half, width))

    def join(bit, own, other):
        return jnp.where(bit == 0, jnp.concatenate([own, other]), jnp.concatenate([other, own]))

    def ring(shift):
        return [(at(zz, yy), at(zz + shift, yy)) for zz in range(n_z) for yy in range(2)]

    pair = join(y, mine, lax.ppermute(mine, "prow", flip_y))
    moved = [pair] + [lax.ppermute(pair, "prow", ring(shift)) for shift in (1, 2, 3)]
    corner = []
    for t in range(steps // 2):
        away = (z - t) % n_z
        corner.append(jnp.where(away == 0, moved[0], jnp.where(away == 1, moved[1], jnp.where(away == 2, moved[2], moved[3]))))
    corner = jnp.concatenate(corner)
    corner = corner, lax.ppermute(corner, "pcol", flip_core)

    both, grid = ("prow", "pcol"), [(x, h, c) for x in range(n_col // 4) for h in range(2) for c in range(2)]

    def device(x, h, c, zz, yy):
        return at(zz, yy) * n_col + x * 4 + h * 2 + c

    whole, parts = None, []
    for first, count in PARTS:
        whole, part = products(blocks, lower, masks, whole, first, count)
        parts.append(part)

    over_m = [(s, d) for s, d in mirror if d < steps]
    over_y = [(s, d) for s, d in flip_y if d < steps]
    over_z = [(s, d) for s, d in flip_z if d < steps]
    routes = (flip_y, flip_z, over_m), (flip_z, over_m, over_y), (mirror, flip_y, over_z)
    pieces = eliminate(masks, parts, corner)
    held = [(pieces[2 * n], pieces[2 * n + 1]) for n in range(len(SIZES))]
    for stage in range(3):
        held = [(lax.ppermute(send, "prow", routes[n][stage]), keep) for n, (send, keep) in enumerate(held)]
        if stage < 2:
            held = [halving(masks, n, stage + 2, keep, came) for n, (came, keep) in enumerate(held)]
    row = masked_row(masks, [v for came, keep in held for v in (keep, came)])

    def turn(k, x, h, c):
        return at(k // 2, k % 2) * n_col + x * 4 + h * 2 + c, device(x, k // 2 % 2, k % 2, x % 2 * 2 + h, c)

    places = [(h, c, zz, yy) for h in range(2) for c in range(2) for zz in range(n_z) for yy in range(2)]

    def slide(place, start, end):
        h, c, zz, yy = place
        return device(start, h, c, zz, yy), device(end, h, c, zz, yy)

    x = q // 4
    first = lax.ppermute(row, both, [turn(k, *place) for k in range(4) for place in grid])
    second = lax.ppermute(row, both, [turn(k, *place) for k in range(4, steps) for place in grid])
    odd0 = lax.ppermute(first, both, [slide(pl_, pl_[2] // 2 + 2, 0) for pl_ in places])
    odd1 = lax.ppermute(second, both, [slide(pl_, pl_[2] // 2 + 2, 1) for pl_ in places if pl_[0] == 0])
    route = [slide(pl_, 0, 1) for pl_ in places if pl_[2] // 2 == 0 and pl_[0] == 0]
    route += [slide(pl_, 1, 0) for pl_ in places if pl_[2] // 2 == 1]
    moved = lax.ppermute(jnp.where(x == 0, second, first), both, route)
    mine = jnp.where(x == 0, first, second)
    values = [row, jnp.where(x == z // 2, mine, moved), jnp.where(x == 0, odd0, odd1)]

    sums = column_products(masks, 0, values[1], lower, ())
    upper, under = column_products(masks, 1, values[2], lower, sums)

    def here(perm):
        return [(s * n_col + d, t * n_col + d) for s, t in perm for d in range(steps)]

    orders = (flip_y, flip_z), (flip_z, mirror), (mirror, flip_y)
    for (one, two) in orders:
        came = lax.ppermute(upper, both, here(one)), lax.ppermute(under, both, here(two))
        upper, under = upper + came[0], under + came[1]
    sums = jnp.concatenate([upper, under])

    def around(t):
        route = []
        for d in range(steps):
            to = (d + t) % steps
            flip = d // 2 % 2 ^ to // 2 % 2
            route += [(s * n_col + d, (s ^ flip) * n_col + to) for s in range(n_row)]
        return route

    turns = [lax.ppermute(sums, both, around(t)) for t in (2, 4)]
    sums = [sums, *turns]
    sums += [lax.ppermute(v, "pcol", [(d, d ^ 1) for d in range(steps)]) for v in sums]
    whole = patch(masks, values, whole)
    whole = corner_blocks(masks, sums, corner, dinv, whole)
    return whole.reshape(ainv_in.shape)


def solution(mesh):
    placed = (
        P(None, "prow", None, "pcol", None, None),
        P(None, "prow", None, None, None),
        P(),
        P(),
    )
    return jax.shard_map(
        per_device,
        mesh=mesh,
        in_specs=placed,
        out_specs=P(None, "prow", None, "pcol", None, None),
        check_vma=False,
    )
```
